32 devices in a mesh: row: 4 (over x, core), col: 8 (over z, y).
Axes of the slice: x: 2, y: 2, z: 4, core: 2. Of those that a mesh axis runs over, the one named last changes fastest.
Arguments:
- tensor: float32 [1024, 32, 1024], P(None, 'row', 'col'), may hold values from -60 to 60, as said below
- factor_two: float32 [32, 32], P('row'), may hold values from -1 to 1
- factor_three: float32 [32, 32], P('col'), may hold values from -1 to 1
- factor_four: float32 [32, 16], replicated, may hold values from -1 to 1
- factor_init: float32 [1024, 64], replicated, may hold values from -6 to 6
Outputs:
- factor_new: float32 [1024, 64], replicated
- core: float32 [64, 32, 32, 16], P(None, 'row', 'col')
The draws below stay inside these ranges and needn't reach their ends.
Inputs may be any that keep to these rules, and one draw needn't show every extreme that they name: `tensor`: scales vary from slab to slab.
All inputs are finite; a program needn't handle non-finite values.
Results may differ from the reference program's by a relative error of at most 0.00013.
Values sent between devices are 32-bit elements; how exact they have to be, the bound alone decides.
A program may use at most 128 MiB of HBM per device.

```python
import jax
import jax.numpy as jnp
from jax import lax

I1 = 1024
I4 = 32
R1 = 64
R2 = 32
R3 = 32
R4 = 16
ITERS = 1
I2 = 32
I3 = 32


def draw_tensor(key, part):
    first, second = jax.random.split(jax.random.fold_in(key, 11), 2)
    shape = (I1, I2, I3 * I4)
    base = jnp.clip(jax.random.normal(first, shape, jnp.float32), -6.0, 6.0)
    ramp_two = jnp.arange(I2, dtype=jnp.float32) / max(I2 - 1, 1)
    ramp_three = jnp.arange(I3, dtype=jnp.float32) / max(I3 - 1, 1)
    logs = jax.random.uniform(second, (I2, I3), jnp.float32) + 0.5 * ramp_two[:, None] + 0.5 * ramp_three[None, :] - 1.0
    scales = jnp.repeat(10.0 ** logs, I4, axis=1)
    values = base * scales[None, :, :]
    return jnp.clip(values, -60.0, 60.0)


def levels(key, dims, cuts, smallest, high):
    loudness = 1.0
    for dim, blocks in cuts:
        draws = jax.random.uniform(jax.random.fold_in(jax.random.fold_in(key, 6), dim), (blocks,), jnp.float32, smallest / len(cuts), high / len(cuts))
        loudness = loudness * jnp.repeat(jnp.exp(draws), dims[dim] // blocks).reshape((-1,) + (1,) * (len(dims) - 1 - dim))
    return loudness


def bell_draw(rng, extent, spread, limit, shards=(), kind=jnp.bfloat16):
    level = levels(rng, extent, shards, -0.22, 0.18) if shards else 1.0
    array = jax.random.normal(rng, extent, jnp.float32) * spread * level
    return jnp.minimum(jnp.maximum(array, -limit), limit).astype(kind)


def setup_inputs(seed: int = 0) -> dict:
    key_list = jax.random.split(jax.random.key(seed), 6)
    tensor = draw_tensor(jax.random.fold_in(key_list[5], 71), 0)
    factor_two = bell_draw(key_list[1], (I2, R2), I2 ** -0.5, 1.0, ((0, 4),), jnp.float32)
    factor_three = bell_draw(key_list[2], (I3, R3), I3 ** -0.5, 1.0, ((0, 8),), jnp.float32)
    factor_four = bell_draw(key_list[3], (I4, R4), I4 ** -0.5, 1.0, (), jnp.float32)
    factor_init = bell_draw(key_list[4], (I1, R1), 1.0, 6.0, (), jnp.float32)
    return dict(tensor=tensor, factor_two=factor_two, factor_three=factor_three, factor_four=factor_four, factor_init=factor_init)


def reference(tensor, factor_two, factor_three, factor_four, factor_init):
    highest = lax.Precision.HIGHEST
    data = tensor.reshape(I1, I2, I3, I4)
    fourth = jnp.einsum('abcd,de->abce', data, factor_four, precision=highest)
    third = jnp.einsum('abce,cf->abfe', fourth, factor_three, precision=highest)
    projected = jnp.einsum('abfe,bg->agfe', third, factor_two, precision=highest)
    unfolded = projected.reshape(I1, R2 * R3 * R4)
    gram = jnp.dot(unfolded.astype(jnp.float32), unfolded.T.astype(jnp.float32), precision=highest, preferred_element_type=jnp.float32)
    basis = factor_init
    for step in range(ITERS):
        image = jnp.dot(gram.astype(jnp.float32), basis.astype(jnp.float32), precision=highest, preferred_element_type=jnp.float32)
        square = jnp.dot(image.T.astype(jnp.float32), image.astype(jnp.float32), precision=highest, preferred_element_type=jnp.float32)
        lower = jnp.linalg.cholesky(square)
        basis = jax.scipy.linalg.solve_triangular(lower, image.T, lower=True).T
    core = jnp.dot(basis.T.astype(jnp.float32), unfolded.astype(jnp.float32), precision=highest, preferred_element_type=jnp.float32)
    return (basis, core.reshape(R1, R2, R3, R4))
```

```python
import functools

import jax
import jax.numpy as jnp
from jax import lax
from jax.experimental import pallas as pl
from jax.experimental.pallas import tpu as pltpu
from jax.sharding import PartitionSpec as P

HIGHEST = lax.Precision.HIGHEST
LANES = 128


def dot(a, b, dims):
    return lax.dot_general(a, b, (dims, ((), ())), precision=HIGHEST, preferred_element_type=jnp.float32)


def inverse_factor(square):
    size = square.shape[0]
    rows = lax.broadcasted_iota(jnp.int32, (size, size), 0)
    cols = lax.broadcasted_iota(jnp.int32, (size, size), 1)
    index = lax.broadcasted_iota(jnp.int32, (size, 1), 0)
    left = square
    right = jnp.where(rows == cols, 1.0, 0.0).astype(jnp.float32)
    for k in range(size):
        scale = lax.rsqrt(left[k:k + 1, k:k + 1])
        column = left[:, k:k + 1] * scale
        pivot_left = left[k:k + 1, :] * scale
        pivot_right = right[k:k + 1, :] * scale
        factor = jnp.where(index > k, column, 0.0)
        left = left - factor * pivot_left
        right = jnp.where(index == k, pivot_right, right - factor * pivot_right)
    return right


def finish_kernel(image_ref, basis_ref, inverse_ref):
    image = image_ref[...]
    inverse = inverse_factor(dot(image, image, ((0,), (0,))))
    inverse_ref[...] = inverse
    basis_ref[...] = dot(image, inverse, ((1,), (1,)))


def finish(image):
    rank = image.shape[1]
    return pl.pallas_call(
        finish_kernel,
        out_shape=(
            jax.ShapeDtypeStruct(image.shape, jnp.float32),
            jax.ShapeDtypeStruct((rank, rank), jnp.float32),
        ),
    )(image)


def place():
    return lax.axis_index("row") * lax.axis_size("col") + lax.axis_index("col")


def greet(devices):
    cols = lax.axis_size("col")
    me = place()
    barrier = pltpu.get_barrier_semaphore()

    def hello(k, carry):
        peer = lax.rem(me + k, devices)
        pl.semaphore_signal(barrier, inc=1, device_id=(peer // cols, lax.rem(peer, cols)), device_id_type=pl.DeviceIdType.MESH)
        return carry

    lax.fori_loop(1, devices, hello, 0)
    pl.semaphore_wait(barrier, devices - 1)


def send_all(devices, source, target, send_sem, recv_sem):
    cols = lax.axis_size("col")
    me = place()

    def send(k, carry):
        peer = lax.rem(me + k, devices)
        pltpu.make_async_remote_copy(
            src_ref=source(peer),
            dst_ref=target.at[me],
            send_sem=send_sem,
            recv_sem=recv_sem,
            device_id=(peer // cols, lax.rem(peer, cols)),
            device_id_type=pl.DeviceIdType.MESH,
        ).start()
        return carry

    lax.fori_loop(1, devices, send, 0)
    whole = target.at[pl.ds(0, devices - 1)]
    pltpu.make_async_copy(whole, whole, send_sem).wait()
    pltpu.make_async_copy(whole, whole, recv_sem).wait()


def swap_kernel(devices, put_ref, out_ref, held, send_sem, recv_sem):
    me = place()
    greet(devices)
    send_all(devices, lambda peer: put_ref.at[peer], held, send_sem, recv_sem)
    held[me] = put_ref[me]
    out_ref[...] = held[...]


def total_kernel(devices, put_ref, out_ref, held, mine, spread, sems):
    me = place()
    greet(devices)
    send_all(devices, lambda peer: put_ref.at[peer], held, sems.at[0], sems.at[1])
    held[me] = put_ref[me]
    mine[...] = jnp.sum(held[...], axis=0)
    send_all(devices, lambda peer: mine, spread, sems.at[2], sems.at[3])
    spread[me] = mine[...]
    out_ref[...] = spread[...]


def swap(values, ident):
    devices = values.shape[0]
    return pl.pallas_call(
        functools.partial(swap_kernel, devices),
        out_shape=jax.ShapeDtypeStruct(values.shape, jnp.float32),
        in_specs=[pl.BlockSpec(memory_space=pltpu.VMEM)],
        out_specs=pl.BlockSpec(memory_space=pltpu.VMEM),
        scratch_shapes=[pltpu.VMEM(values.shape, jnp.float32), pltpu.SemaphoreType.DMA, pltpu.SemaphoreType.DMA],
        compiler_params=pltpu.CompilerParams(collective_id=ident, has_side_effects=True),
    )(values)


def total(values, ident):
    devices = values.shape[0]
    return pl.pallas_call(
        functools.partial(total_kernel, devices),
        out_shape=jax.ShapeDtypeStruct(values.shape, jnp.float32),
        in_specs=[pl.BlockSpec(memory_space=pltpu.VMEM)],
        out_specs=pl.BlockSpec(memory_space=pltpu.VMEM),
        scratch_shapes=[
            pltpu.VMEM(values.shape, jnp.float32),
            pltpu.VMEM(values.shape[1:], jnp.float32),
            pltpu.VMEM(values.shape, jnp.float32),
            pltpu.SemaphoreType.DMA((4,)),
        ],
        compiler_params=pltpu.CompilerParams(collective_id=ident, has_side_effects=True),
    )(values)


def split(x):
    high = x.astype(jnp.bfloat16)
    return high, (x - high.astype(jnp.float32)).astype(jnp.bfloat16)


def narrow(a, b, dims=((1,), (0,))):
    return lax.dot_general(a, b, (dims, ((), ())), preferred_element_type=jnp.float32)


def left_split(x, high, low):
    rows = x.shape[0]
    top, rest = split(x)
    both = narrow(jnp.concatenate([top, rest], axis=0), high)
    return both[:rows] + both[rows:] + narrow(top, low)


def iota(shape, dim):
    return lax.broadcasted_iota(jnp.int32, shape, dim)


def ones_where(mask):
    return jnp.where(mask, 1.0, 0.0).astype(jnp.float32)


def expand_rows(square, copies):
    size = square.shape[0] * copies
    pick = ones_where(iota((size, square.shape[0]), 0) // copies == iota((size, square.shape[0]), 1))
    pick_right = ones_where(iota((square.shape[1], square.shape[1] * copies), 1) // copies == iota((square.shape[1], square.shape[1] * copies), 0))
    wide = dot(dot(pick, square, ((1,), (0,))), pick_right, ((1,), (0,)))
    return jnp.where(iota(wide.shape, 0) % copies == iota(wide.shape, 1) % copies, wide, 0.0)


def store_lanes(matrix, copies, high_ref, low_ref):
    width = matrix.shape[1] * copies
    pick = ones_where(iota((matrix.shape[1], width), 1) // copies == iota((matrix.shape[1], width), 0))
    wide = dot(matrix, pick, ((1,), (0,)))
    keep = iota((copies, width), 1) % copies == iota((copies, width), 0)
    for k in range(matrix.shape[0]):
        rows = jnp.where(keep, jnp.broadcast_to(wide[k:k + 1, :], (copies, width)), 0.0)
        high, low = split(rows)
        high_ref[k * copies:(k + 1) * copies, :] = high
        low_ref[k * copies:(k + 1) * copies, :] = low


def send_to(source, target, peer, send_sem, recv_sem):
    cols = lax.axis_size("col")
    pltpu.make_async_remote_copy(
        src_ref=source,
        dst_ref=target,
        send_sem=send_sem,
        recv_sem=recv_sem,
        device_id=(peer // cols, lax.rem(peer, cols)),
        device_id_type=pl.DeviceIdType.MESH,
    ).start()


def wait_all(ref, count, sem):
    whole = ref.at[pl.ds(0, count)]
    pltpu.make_async_copy(whole, whole, sem).wait()


def hooi_kernel(devices, tensor_ref, two_ref, three_ref, four_ref, init_ref, core_ref, basis_ref,
                slabs, high_ref, low_ref, mix_high, mix_low, hat_high, hat_low, turn_high, turn_low,
                lane_high, lane_low, twos, threes, puts, gots, put_image, got_image, mine, spread,
                load_sem, send_sem, recv_sem, axis_sem):
    rows, cols = lax.axis_size("row"), lax.axis_size("col")
    row, col = lax.axis_index("row"), lax.axis_index("col")
    me = place()
    rank_one, first_len = init_ref.shape
    local_two, local_three = two_ref.shape[0], three_ref.shape[0]
    rank_four, fourth_len = four_ref.shape
    width = local_three * fourth_len
    lanes = local_two * rank_four
    pairs = local_two * local_three
    copies = rank_one // devices
    features = pairs * rank_four
    tile = local_three * copies

    loads = [pltpu.make_async_copy(tensor_ref.at[:, b, :], slabs.at[b], load_sem.at[b]) for b in range(local_two)]
    for load in loads:
        load.start()

    barrier = pltpu.get_barrier_semaphore()

    def hello(k, carry):
        peer = lax.rem(me + k, devices)
        pl.semaphore_signal(barrier, inc=1, device_id=(peer // cols, lax.rem(peer, cols)), device_id_type=pl.DeviceIdType.MESH)
        return carry

    lax.fori_loop(1, devices, hello, 0)

    lane = iota((fourth_len, features), 1)
    pick = ones_where(iota((rank_four, features), 1) % rank_four == iota((rank_four, features), 0))
    four = dot(four_ref[...], pick, ((0,), (0,)))
    four_high = four.astype(jnp.bfloat16).astype(jnp.float32)
    four_low = four - four_high
    for b in range(local_two):
        for c in range(local_three):
            keep = lane // rank_four == c * local_two + b
            part = slice((b * local_three + c) * fourth_len, (b * local_three + c + 1) * fourth_len)
            mix_high[part, :] = jnp.where(keep, four_high, 0.0).astype(jnp.bfloat16)
            mix_low[part, :] = jnp.where(keep, four_low, 0.0).astype(jnp.bfloat16)

    init_high, init_low = split(init_ref[...])
    init_both = jnp.concatenate([init_high, init_low], axis=0)
    pulled = []
    step = 2 if local_two % 2 == 0 else 1
    for b in range(0, local_two, step):
        for k in range(b, b + step):
            loads[k].wait()
            high, low = split(slabs[k])
            high_ref[:, k * width:(k + 1) * width] = high
            low_ref[:, k * width:(k + 1) * width] = low
        part = slice(b * width, (b + step) * width)
        both = narrow(init_both, high_ref[:, part])
        pulled.append(both[:rank_one] + both[rank_one:] + narrow(init_high, low_ref[:, part]))
    vectors = left_split(jnp.concatenate(pulled, axis=1), mix_high[...], mix_low[...])

    def deal(vectors, put):
        for c in range(local_three):
            for k in range(copies):
                put[pl.ds(c * copies + k, devices, stride=tile), :] = vectors[k * devices:(k + 1) * devices, c * lanes:(c + 1) * lanes]

    def collect(got):
        return jnp.concatenate([
            jnp.concatenate([got[pl.ds(c * copies + k, devices, stride=tile), :] for k in range(copies)], axis=0)
            for c in range(local_three)], axis=1)

    def exchange(stage):
        put, got = puts.at[stage], gots.at[stage]

        def send(k, carry):
            peer = lax.rem(me + k, devices)
            send_to(put.at[pl.ds(pl.multiple_of(peer * tile, tile), tile)], got.at[pl.ds(pl.multiple_of(me * tile, tile), tile)], peer, send_sem.at[stage], recv_sem.at[stage])
            return carry

        lax.fori_loop(1, devices, send, 0)
        here = pl.ds(pl.multiple_of(me * tile, tile), tile)
        got[here, :] = put[here, :]

    def arrive(stage):
        wait_all(gots.at[stage], (devices - 1) * tile, recv_sem.at[stage])

    def block(stage):
        got = gots.at[stage]
        return jnp.concatenate([got[k * cols * tile:(k + 1) * cols * tile, :] for k in range(rows)], axis=1)

    def contract(stage, matrix):
        high, low = split(matrix)
        both = jnp.concatenate([high, low], axis=0)
        size = matrix.shape[0]
        top, rest = split(block(stage))
        mixed = narrow(both, top)
        mixed = mixed[:size] + mixed[size:] + narrow(high, rest)
        return left_split(mixed, lane_high[...], lane_low[...])

    def lay(result, stage):
        for k in range(rows):
            puts[stage, k * cols * tile:(k + 1) * cols * tile, :] = result[:, k * lanes:(k + 1) * lanes]

    deal(vectors, puts.at[0])
    pl.semaphore_wait(barrier, devices - 1)

    def send_two(k, carry):
        other = lax.rem(row + k, rows)
        send_to(two_ref, twos.at[row], other * cols + col, axis_sem.at[0], axis_sem.at[1])
        return carry

    def send_three(k, carry):
        other = lax.rem(col + k, cols)
        send_to(three_ref, threes.at[col], row * cols + other, axis_sem.at[2], axis_sem.at[3])
        return carry

    lax.fori_loop(1, rows, send_two, 0)
    lax.fori_loop(1, cols, send_three, 0)
    exchange(0)
    twos[row] = two_ref[...]
    threes[col] = three_ref[...]

    count = 4
    piece = first_len // count
    for k in range(count):
        part = slice(k * piece, (k + 1) * piece)
        hat = narrow(high_ref[part, :], mix_high[...]) + narrow(high_ref[part, :], mix_low[...]) + narrow(low_ref[part, :], mix_high[...])
        high, low = split(hat)
        hat_high[part, :] = high
        hat_low[part, :] = low
        turned = hat.T
        high, low = split(turned)
        turn_high[:, part] = high
        turn_low[:, part] = low

    wait_all(twos, rows - 1, axis_sem.at[1])
    wait_all(threes, cols - 1, axis_sem.at[3])
    whole_two = jnp.concatenate([twos[k] for k in range(rows)], axis=0)
    whole_three = jnp.concatenate([threes[k] for k in range(cols)], axis=0)
    store_lanes(dot(whole_two, whole_two, ((1,), (1,))), rank_four, lane_high, lane_low)
    left = expand_rows(dot(whole_three, whole_three, ((1,), (1,))), copies)

    arrive(0)
    lay(contract(0, left), 1)
    exchange(1)
    store_lanes(whole_two, rank_four, lane_high, lane_low)
    left = expand_rows(whole_three.T, copies)
    arrive(1)

    image = left_split(collect(gots.at[1]), turn_high[...], turn_low[...])
    high_tiles = rank_one // 8
    wide_tiles = first_len // LANES
    each = high_tiles * wide_tiles // devices
    spans = wide_tiles // each
    for i in range(devices):
        for j in range(each):
            r, w = i // spans, (i % spans) * each + j
            put_image[i, j] = image[r * 8:(r + 1) * 8, w * LANES:(w + 1) * LANES]

    def scatter(k, carry):
        peer = lax.rem(me + k, devices)
        send_to(put_image.at[peer], got_image.at[me], peer, send_sem.at[4], recv_sem.at[4])
        return carry

    lax.fori_loop(1, devices, scatter, 0)
    got_image[me] = put_image[me]
    wait_all(got_image, devices - 1, recv_sem.at[4])
    mine[...] = jnp.sum(got_image[...], axis=0)

    def share(k, carry):
        peer = lax.rem(me + k, devices)
        send_to(mine, spread.at[me], peer, send_sem.at[5], recv_sem.at[5])
        return carry

    lax.fori_loop(1, devices, share, 0)
    spread[me] = mine[...]
    wait_all(spread, devices - 1, recv_sem.at[5])
    image = jnp.concatenate([
        jnp.concatenate([spread[r * spans + k, j] for k in range(spans) for j in range(each)], axis=1)
        for r in range(high_tiles)], axis=0)

    deal(left_split(image, hat_high[...], hat_low[...]), puts.at[2])
    exchange(2)
    inverse = inverse_factor(dot(image, image, ((1,), (1,))))
    arrive(2)
    lay(contract(2, left), 3)
    exchange(3)
    basis_ref[...] = dot(inverse, image, ((1,), (0,)))
    arrive(3)
    core = dot(collect(gots.at[3]), inverse, ((0,), (1,)))
    for c in range(local_three):
        for b in range(local_two):
            core_ref[b, c] = core[(c * local_two + b) * rank_four:(c * local_two + b + 1) * rank_four, :]

    for stage in range(4):
        wait_all(puts.at[stage], (devices - 1) * tile, send_sem.at[stage])
    wait_all(put_image, devices - 1, send_sem.at[4])
    wait_all(spread, devices - 1, send_sem.at[5])
    wait_all(twos, rows - 1, axis_sem.at[0])
    wait_all(threes, cols - 1, axis_sem.at[2])


def fits(tensor, factor_two, factor_three, factor_four, factor_init):
    rows, cols = lax.axis_size("row"), lax.axis_size("col")
    devices = rows * cols
    first_len, local_two, width = tensor.shape
    fourth_len, rank_four = factor_four.shape
    rank_one = factor_init.shape[1]
    local_three = width // fourth_len
    same = factor_two.shape[1] == local_two * rows and factor_three.shape[1] == local_three * cols
    even = rank_one % (8 * devices // local_three) == 0 and rank_one % devices == 0 and local_three * (rank_one // devices) == 8
    flat = local_two * rank_four == LANES and width == LANES and first_len % LANES == 0
    tiles = (rank_one // 8) * (first_len // LANES)
    return same and even and flat and tiles % devices == 0 and (first_len // LANES) % max(tiles // devices, 1) == 0


def fused(tensor, factor_two, factor_three, factor_four, factor_init):
    rows, cols = lax.axis_size("row"), lax.axis_size("col")
    devices = rows * cols
    first_len, local_two, width = tensor.shape
    fourth_len, rank_four = factor_four.shape
    rank_one = factor_init.shape[1]
    local_three = width // fourth_len
    features = local_two * local_three * rank_four
    total_width = local_two * width
    tile = local_three * (rank_one // devices)
    lanes = local_two * rank_four
    each = (rank_one // 8) * (first_len // LANES) // devices
    wide = rows * lanes
    f32, bf16 = jnp.float32, jnp.bfloat16
    vmem = pl.BlockSpec(memory_space=pltpu.VMEM)
    core, basis = pl.pallas_call(
        functools.partial(hooi_kernel, devices),
        out_shape=(
            jax.ShapeDtypeStruct((local_two, local_three, rank_four, rank_one), f32),
            jax.ShapeDtypeStruct((rank_one, first_len), f32),
        ),
        in_specs=[pl.BlockSpec(memory_space=pl.ANY), vmem, vmem, vmem, vmem],
        out_specs=(vmem, vmem),
        scratch_shapes=[
            pltpu.VMEM((local_two, first_len, width), f32),
            pltpu.VMEM((first_len, total_width), bf16),
            pltpu.VMEM((first_len, total_width), bf16),
            pltpu.VMEM((total_width, features), bf16),
            pltpu.VMEM((total_width, features), bf16),
            pltpu.VMEM((first_len, features), bf16),
            pltpu.VMEM((first_len, features), bf16),
            pltpu.VMEM((features, first_len), bf16),
            pltpu.VMEM((features, first_len), bf16),
            pltpu.VMEM((wide, wide), bf16),
            pltpu.VMEM((wide, wide), bf16),
            pltpu.VMEM((rows,) + factor_two.shape, f32),
            pltpu.VMEM((cols,) + factor_three.shape, f32),
            pltpu.VMEM((4, devices * tile, lanes), f32),
            pltpu.VMEM((4, devices * tile, lanes), f32),
            pltpu.VMEM((devices, each, 8, LANES), f32),
            pltpu.VMEM((devices, each, 8, LANES), f32),
            pltpu.VMEM((each, 8, LANES), f32),
            pltpu.VMEM((devices, each, 8, LANES), f32),
            pltpu.SemaphoreType.DMA((local_two,)),
            pltpu.SemaphoreType.DMA((6,)),
            pltpu.SemaphoreType.DMA((6,)),
            pltpu.SemaphoreType.DMA((4,)),
        ],
        compiler_params=pltpu.CompilerParams(collective_id=0, has_side_effects=True),
    )(tensor, factor_two, factor_three, factor_four.T, factor_init.T)
    return basis.T, core.transpose(3, 0, 1, 2)


def shards(tensor, factor_two, factor_three, factor_four, factor_init):
    if fits(tensor, factor_two, factor_three, factor_four, factor_init):
        return fused(tensor, factor_two, factor_three, factor_four, factor_init)
    axes = ("row", "col")
    first_len, local_two, width = tensor.shape
    fourth_len, rank_four = factor_four.shape
    local_three = width // fourth_len
    rank_one = factor_init.shape[1]
    rows, cols = lax.axis_size("row"), lax.axis_size("col")
    devices = rows * cols
    local_pairs = local_two * local_three
    features = rank_four * rank_one
    part = features // devices
    data = tensor.reshape(first_len, local_pairs, fourth_len)
    rank_two, rank_three = factor_two.shape[1], factor_three.shape[1]

    def pull(vectors):
        mixed = jnp.einsum("apd,ar->prd", data, vectors, precision=lax.Precision.HIGH)
        return jnp.einsum("prd,de->per", mixed, factor_four, precision=HIGHEST).reshape(local_pairs, features)

    def share(values, ident):
        length = values.shape[1]
        padded = -(-length // LANES) * LANES
        values = jnp.pad(values, ((0, 0), (0, padded - length))).reshape(devices, padded // LANES, LANES)
        return swap(values, ident).reshape(devices, padded)[:, :length]

    def spread(block, ident, extra=None):
        put = block.reshape(local_pairs, devices, part).transpose(1, 0, 2).reshape(devices, local_pairs * part)
        if extra is not None:
            put = jnp.concatenate([put, jnp.broadcast_to(extra[None], (devices, extra.shape[0]))], axis=1)
        got = share(put, ident)
        rest = got[:, local_pairs * part:]
        got = got[:, :local_pairs * part]
        got = got.reshape(rows, cols, local_two, local_three, part)
        return got.transpose(0, 2, 1, 3, 4).reshape(rows * local_two, cols * local_three, part), rest

    def gather(block, ident):
        two, three, _ = block.shape
        put = block.reshape(rows, two // rows, cols, three // cols, part).transpose(0, 2, 1, 3, 4)
        got = share(put.reshape(devices, -1), ident).reshape(devices, (two // rows) * (three // cols), part)
        return got.transpose(1, 0, 2).reshape(got.shape[1], features)

    extra = jnp.concatenate([factor_two.reshape(-1), factor_three.reshape(-1)])
    block, rest = spread(pull(factor_init), 1, extra)
    rest = rest.reshape(rows, cols, -1)
    whole_two = rest[:, 0, :factor_two.size].reshape(-1, rank_two)
    whole_three = rest[0, :, factor_two.size:].reshape(-1, rank_three)
    block = jnp.einsum("bcq,bg->gcq", block, whole_two, precision=HIGHEST)
    block = jnp.einsum("gcq,cf->gfq", block, whole_three, precision=HIGHEST)
    block = jnp.einsum("gfq,cf->gcq", block, whole_three, precision=HIGHEST)
    block = jnp.einsum("gcq,bg->bcq", block, whole_two, precision=HIGHEST)
    block = gather(block, 2).reshape(local_pairs, rank_four, rank_one)
    block = jnp.einsum("per,de->pdr", block, factor_four, precision=HIGHEST)
    image = jnp.dot(tensor.reshape(first_len, -1), block.reshape(-1, rank_one), precision=lax.Precision.HIGH)
    half = first_len // 2
    image = jnp.concatenate([image[:half], image[half:]], axis=1).reshape(devices, half // devices, 2 * rank_one)
    image = total(image, 0).reshape(half, 2 * rank_one)
    image = jnp.concatenate([image[:, :rank_one], image[:, rank_one:]], axis=0)
    basis, inverse = finish(image)
    block, _ = spread(pull(image), 3)
    block = jnp.einsum("bcq,bg->gcq", block, whole_two, precision=HIGHEST)
    block = jnp.einsum("gcq,cf->gfq", block, whole_three, precision=HIGHEST)
    block = gather(block, 4).reshape(-1, rank_four, rank_one)
    core = jnp.einsum("per,sr->spe", block, inverse, precision=HIGHEST)
    return (basis, core.reshape(rank_one, rank_two // rows, rank_three // cols, rank_four))


def solution(mesh):
    in_specs = (P(None, "row", "col"), P("row", None), P("col", None), P(), P())
    out_specs = (P(), P(None, "row", "col", None))
    return jax.shard_map(shards, mesh=mesh, in_specs=in_specs, out_specs=out_specs, check_vma=False)
```

```python
import functools

import jax
import jax.numpy as jnp
from jax import lax
from jax.experimental import pallas as pl
from jax.experimental.pallas import tpu as pltpu
from jax.sharding import PartitionSpec as P

HIGHEST = lax.Precision.HIGHEST
LANES = 128


def dot(a, b, dims):
    return lax.dot_general(a, b, (dims, ((), ())), precision=HIGHEST, preferred_element_type=jnp.float32)


def inverse_factor(square):
    size = square.shape[0]
    rows = lax.broadcasted_iota(jnp.int32, (size, size), 0)
    cols = lax.broadcasted_iota(jnp.int32, (size, size), 1)
    index = lax.broadcasted_iota(jnp.int32, (size, 1), 0)
    left = square
    right = jnp.where(rows == cols, 1.0, 0.0).astype(jnp.float32)
    for k in range(size):
        scale = lax.rsqrt(left[k:k + 1, k:k + 1])
        column = left[:, k:k + 1] * scale
        pivot_left = left[k:k + 1, :] * scale
        pivot_right = right[k:k + 1, :] * scale
        factor = jnp.where(index > k, column, 0.0)
        left = left - factor * pivot_left
        right = jnp.where(index == k, pivot_right, right - factor * pivot_right)
    return right


def finish_kernel(image_ref, basis_ref, inverse_ref):
    image = image_ref[...]
    inverse = inverse_factor(dot(image, image, ((0,), (0,))))
    inverse_ref[...] = inverse
    basis_ref[...] = dot(image, inverse, ((1,), (1,)))


def finish(image):
    rank = image.shape[1]
    return pl.pallas_call(
        finish_kernel,
        out_shape=(
            jax.ShapeDtypeStruct(image.shape, jnp.float32),
            jax.ShapeDtypeStruct((rank, rank), jnp.float32),
        ),
    )(image)


def place():
    return lax.axis_index("row") * lax.axis_size("col") + lax.axis_index("col")


def greet(devices):
    cols = lax.axis_size("col")
    me = place()
    barrier = pltpu.get_barrier_semaphore()

    def hello(k, carry):
        peer = lax.rem(me + k, devices)
        pl.semaphore_signal(barrier, inc=1, device_id=(peer // cols, lax.rem(peer, cols)), device_id_type=pl.DeviceIdType.MESH)
        return carry

    lax.fori_loop(1, devices, hello, 0)
    pl.semaphore_wait(barrier, devices - 1)


def send_all(devices, source, target, send_sem, recv_sem):
    cols = lax.axis_size("col")
    me = place()

    def send(k, carry):
        peer = lax.rem(me + k, devices)
        pltpu.make_async_remote_copy(
            src_ref=source(peer),
            dst_ref=target.at[me],
            send_sem=send_sem,
            recv_sem=recv_sem,
            device_id=(peer // cols, lax.rem(peer, cols)),
            device_id_type=pl.DeviceIdType.MESH,
        ).start()
        return carry

    lax.fori_loop(1, devices, send, 0)
    whole = target.at[pl.ds(0, devices - 1)]
    pltpu.make_async_copy(whole, whole, send_sem).wait()
    pltpu.make_async_copy(whole, whole, recv_sem).wait()


def swap_kernel(devices, put_ref, out_ref, held, send_sem, recv_sem):
    me = place()
    greet(devices)
    send_all(devices, lambda peer: put_ref.at[peer], held, send_sem, recv_sem)
    held[me] = put_ref[me]
    out_ref[...] = held[...]


def total_kernel(devices, put_ref, out_ref, held, mine, spread, sems):
    me = place()
    greet(devices)
    send_all(devices, lambda peer: put_ref.at[peer], held, sems.at[0], sems.at[1])
    held[me] = put_ref[me]
    mine[...] = jnp.sum(held[...], axis=0)
    send_all(devices, lambda peer: mine, spread, sems.at[2], sems.at[3])
    spread[me] = mine[...]
    out_ref[...] = spread[...]


def swap(values, ident):
    devices = values.shape[0]
    return pl.pallas_call(
        functools.partial(swap_kernel, devices),
        out_shape=jax.ShapeDtypeStruct(values.shape, jnp.float32),
        in_specs=[pl.BlockSpec(memory_space=pltpu.VMEM)],
        out_specs=pl.BlockSpec(memory_space=pltpu.VMEM),
        scratch_shapes=[pltpu.VMEM(values.shape, jnp.float32), pltpu.SemaphoreType.DMA, pltpu.SemaphoreType.DMA],
        compiler_params=pltpu.CompilerParams(collective_id=ident, has_side_effects=True),
    )(values)


def total(values, ident):
    devices = values.shape[0]
    return pl.pallas_call(
        functools.partial(total_kernel, devices),
        out_shape=jax.ShapeDtypeStruct(values.shape, jnp.float32),
        in_specs=[pl.BlockSpec(memory_space=pltpu.VMEM)],
        out_specs=pl.BlockSpec(memory_space=pltpu.VMEM),
        scratch_shapes=[
            pltpu.VMEM(values.shape, jnp.float32),
            pltpu.VMEM(values.shape[1:], jnp.float32),
            pltpu.VMEM(values.shape, jnp.float32),
            pltpu.SemaphoreType.DMA((4,)),
        ],
        compiler_params=pltpu.CompilerParams(collective_id=ident, has_side_effects=True),
    )(values)


def split(x):
    high = x.astype(jnp.bfloat16)
    return high, (x - high.astype(jnp.float32)).astype(jnp.bfloat16)


def narrow(a, b):
    return lax.dot_general(a, b, (((1,), (0,)), ((), ())), preferred_element_type=jnp.float32)


def left_split(x, high, low):
    rows = x.shape[0]
    top, rest = split(x)
    both = narrow(jnp.concatenate([top, rest], axis=0), high)
    return both[:rows] + both[rows:] + narrow(top, low)


def iota(shape, dim):
    return lax.broadcasted_iota(jnp.int32, shape, dim)


def ones_where(mask):
    return jnp.where(mask, 1.0, 0.0).astype(jnp.float32)


def expand_rows(square, copies):
    tall = (square.shape[0] * copies, square.shape[0])
    wide = (square.shape[1], square.shape[1] * copies)
    result = dot(ones_where(iota(tall, 0) // copies == iota(tall, 1)), square, ((1,), (0,)))
    result = dot(result, ones_where(iota(wide, 1) // copies == iota(wide, 0)), ((1,), (0,)))
    return jnp.where(iota(result.shape, 0) % copies == iota(result.shape, 1) % copies, result, 0.0)


def store_lanes(matrix, copies, high_ref, low_ref):
    shape = (matrix.shape[1], matrix.shape[1] * copies)
    wide = dot(matrix, ones_where(iota(shape, 1) // copies == iota(shape, 0)), ((1,), (0,)))
    shape = (copies, shape[1])
    keep = iota(shape, 1) % copies == iota(shape, 0)
    for k in range(matrix.shape[0]):
        high, low = split(jnp.where(keep, jnp.broadcast_to(wide[k:k + 1, :], shape), 0.0))
        high_ref[k * copies:(k + 1) * copies, :] = high
        low_ref[k * copies:(k + 1) * copies, :] = low


def eliminate(left, right, first, last):
    size = left.shape[0]
    index = iota((size, 1), 0)
    for k in range(first, last):
        scale = lax.rsqrt(left[k:k + 1, k:k + 1])
        column = left[:, k:k + 1] * scale
        pivot_left = left[k:k + 1, :] * scale
        pivot_right = right[k:k + 1, :] * scale
        factor = jnp.where(index > k, column, 0.0)
        left = left - factor * pivot_left
        right = jnp.where(index == k, pivot_right, right - factor * pivot_right)
    return left, right


def copy_to(source, target, row, col, send_sem, recv_sem):
    pltpu.make_async_remote_copy(
        src_ref=source,
        dst_ref=target,
        send_sem=send_sem,
        recv_sem=recv_sem,
        device_id=(row, col),
        device_id_type=pl.DeviceIdType.MESH,
    ).start()


def wait_for(ref, sem):
    pltpu.make_async_copy(ref, ref, sem).wait()


def hooi_kernel(tensor_hbm, two_hbm, three_hbm, four_hbm, init_hbm, core_ref, basis_ref,
                slabs, two_ref, three_ref, four_ref, init_ref,
                high_ref, low_ref, mix_high, mix_low, hat_high, hat_low, turn_high, turn_low,
                lane_high, lane_low, twos, threes, deals, dealt, backs, backed,
                parts, paired, sums, shares, mine, spread,
                load_sem, factor_sem, send_sem, deal_sem, back_sem, image_sem):
    rows, cols = lax.axis_size("row"), lax.axis_size("col")
    row, col = lax.axis_index("row"), lax.axis_index("col")
    devices = rows * cols
    members = devices // 2
    half = lax.rem(row, 2)
    seat = (row // 2) * cols + col
    me = row * cols + col
    partner = row + 1 - 2 * half
    rank_one, first_len = init_ref.shape
    half_rank = rank_one // 2
    local_two, local_three = two_ref.shape[0], three_ref.shape[0]
    rank_four, fourth_len = four_ref.shape
    width = local_three * fourth_len
    lanes = local_two * rank_four
    features = local_three * lanes
    copies = rank_one // devices
    tile = local_three * copies
    each = sums.shape[2]

    slab_loads = [pltpu.make_async_copy(tensor_hbm.at[:, b, :], slabs.at[b], load_sem.at[b]) for b in range(local_two)]
    small = [(four_hbm, four_ref), (init_hbm, init_ref), (two_hbm, two_ref), (three_hbm, three_ref)]
    small_loads = [pltpu.make_async_copy(source, target, load_sem.at[local_two + k]) for k, (source, target) in enumerate(small)]
    small_loads[0].start()
    small_loads[1].start()
    for load in slab_loads:
        load.start()
    small_loads[2].start()
    small_loads[3].start()

    barrier = pltpu.get_barrier_semaphore()

    def hello(k, carry):
        peer = lax.rem(me + k, devices)
        pl.semaphore_signal(barrier, inc=1, device_id=(peer // cols, lax.rem(peer, cols)), device_id_type=pl.DeviceIdType.MESH)
        return carry

    lax.fori_loop(1, devices, hello, 0)

    def target(k):
        turn = k // (rows // 2)
        shift = (turn + 1) // 2
        there = lax.rem(col + cols // 2 + cols + (1 - 2 * lax.rem(turn, 2)) * shift, cols)
        return lax.rem(row // 2 + rows - 1 - lax.rem(k, rows // 2), rows // 2), there

    def at(index, count):
        return pl.ds(pl.multiple_of(index * count, count), count)

    small_loads[0].wait()
    lane = iota((fourth_len, features), 1)
    shape = (rank_four, features)
    four = dot(four_ref[...], ones_where(iota(shape, 1) % rank_four == iota(shape, 0)), ((0,), (0,)))
    four_high = four.astype(jnp.bfloat16).astype(jnp.float32)
    four_low = four - four_high
    for b in range(local_two):
        for c in range(local_three):
            keep = lane // rank_four == c * local_two + b
            part = slice((b * local_three + c) * fourth_len, (b * local_three + c + 1) * fourth_len)
            mix_high[part, :] = jnp.where(keep, four_high, 0.0).astype(jnp.bfloat16)
            mix_low[part, :] = jnp.where(keep, four_low, 0.0).astype(jnp.bfloat16)

    small_loads[1].wait()
    init_high, init_low = split(init_ref[...])
    init_both = jnp.concatenate([init_high, init_low], axis=0)
    group = 2 if local_two % 2 == 0 else 1

    def pull_group(b):
        part = slice(b * width, (b + group) * width)
        both = narrow(init_both, high_ref[:, part])
        pulled = both[:rank_one] + both[rank_one:] + narrow(init_high, low_ref[:, part])
        return left_split(pulled, mix_high[part, :], mix_low[part, :])

    vectors = None
    for b in range(0, local_two, group):
        for k in range(b, b + group):
            slab_loads[k].wait()
            high, low = split(slabs[k])
            high_ref[:, k * width:(k + 1) * width] = high
            low_ref[:, k * width:(k + 1) * width] = low
        if b > 0:
            more = pull_group(b - group)
            vectors = more if vectors is None else vectors + more
    more = pull_group(local_two - group)
    vectors = more if vectors is None else vectors + more

    def deal(vectors, put):
        for c in range(local_three):
            for k in range(copies):
                put[pl.ds(c * copies + k, members, stride=tile), :] = vectors[k * members:(k + 1) * members, c * lanes:(c + 1) * lanes]

    def send_deal(stage, h):
        def send(k, carry):
            there_row, there_col = target(k)
            copy_to(deals.at[stage, h, at(there_row * cols + there_col, tile)], dealt.at[stage, at(me, tile)],
                    there_row * 2 + h, there_col, send_sem.at[stage], deal_sem.at[stage])
            return carry

        lax.fori_loop(0, members - jnp.where(half == h, 1, 0), send, 0)

    def wait_deal(stage):
        dealt[stage, at(me, tile), :] = deals[stage, half, at(seat, tile), :]
        wait_for(dealt.at[stage, pl.ds(0, (devices - 1) * tile)], deal_sem.at[stage])

    def contract(stage, matrix):
        high, low = split(matrix)
        size = matrix.shape[0]
        block = jnp.concatenate([dealt[stage, k * cols * tile:(k + 1) * cols * tile, :] for k in range(rows)], axis=1)
        top, rest = split(block)
        mixed = narrow(jnp.concatenate([high, low], axis=0), top)
        mixed = mixed[:size] + mixed[size:] + narrow(high, rest)
        result = left_split(mixed, lane_high[...], lane_low[...])
        for k in range(rows):
            backs[stage, k * cols * tile:(k + 1) * cols * tile, :] = result[:, k * lanes:(k + 1) * lanes]

    def send_back(stage):
        def send(k, carry):
            there_row, there_col = target(k)
            for h in range(2):
                copy_to(backs.at[stage, at((there_row * 2 + h) * cols + there_col, tile)], backed.at[stage, half, at(seat, tile)],
                        there_row * 2 + h, there_col, send_sem.at[2 + stage], back_sem.at[stage, half])
            return carry

        lax.fori_loop(0, members - 1, send, 0)
        copy_to(backs.at[stage, at(partner * cols + col, tile)], backed.at[stage, half, at(seat, tile)],
                partner, col, send_sem.at[2 + stage], back_sem.at[stage, half])
        backed[stage, half, at(seat, tile), :] = backs[stage, at(me, tile), :]

    def wait_back(stage, h):
        @pl.when(half == h)
        def _():
            wait_for(backed.at[stage, h, pl.ds(0, (members - 1) * tile)], back_sem.at[stage, h])

        @pl.when(half != h)
        def _():
            wait_for(backed.at[stage, h], back_sem.at[stage, h])

    def collect(stage, h):
        return jnp.concatenate([
            jnp.concatenate([backed[stage, h, pl.ds(c * copies + k, members, stride=tile), :] for k in range(copies)], axis=0)
            for c in range(local_three)], axis=1)

    for h in range(2):
        deal(vectors[h * half_rank:(h + 1) * half_rank], deals.at[0, h])
    small_loads[2].wait()
    small_loads[3].wait()
    pl.semaphore_wait(barrier, devices - 1)

    send_deal(0, 0)
    send_deal(0, 1)

    def send_two(k, carry):
        copy_to(two_ref, twos.at[row], lax.rem(row + k, rows), col, factor_sem.at[0], factor_sem.at[1])
        return carry

    def send_three(k, carry):
        copy_to(three_ref, threes.at[col], row, lax.rem(col + k, cols), factor_sem.at[2], factor_sem.at[3])
        return carry

    lax.fori_loop(1, rows, send_two, 0)
    lax.fori_loop(1, cols, send_three, 0)
    twos[row] = two_ref[...]
    threes[col] = three_ref[...]

    def hat_piece(k, count):
        part = slice(k * first_len // count, (k + 1) * first_len // count)
        hat = narrow(high_ref[part, :], mix_high[...]) + narrow(high_ref[part, :], mix_low[...]) + narrow(low_ref[part, :], mix_high[...])
        hat_high[part, :], hat_low[part, :] = split(hat)
        turn_high[:, part], turn_low[:, part] = split(hat.T)

    hat_piece(0, 4)
    hat_piece(1, 4)
    wait_for(twos.at[pl.ds(0, rows - 1)], factor_sem.at[1])
    wait_for(threes.at[pl.ds(0, cols - 1)], factor_sem.at[3])
    whole_two = jnp.concatenate([twos[k] for k in range(rows)], axis=0)
    whole_three = jnp.concatenate([threes[k] for k in range(cols)], axis=0)
    store_lanes(dot(whole_two, whole_two, ((1,), (1,))), rank_four, lane_high, lane_low)
    left = expand_rows(dot(whole_three, whole_three, ((1,), (1,))), copies)

    wait_deal(0)
    contract(0, left)
    send_back(0)
    hat_piece(2, 4)
    hat_piece(3, 4)

    spans = first_len // LANES // each
    for h in range(2):
        wait_back(0, h)
        image = left_split(collect(0, h), turn_high[...], turn_low[...])
        for i in range(devices):
            for j in range(each):
                r, w = i // spans, (i % spans) * each + j
                parts[h, i // members, i % members, j] = image[r * 8:(r + 1) * 8, w * LANES:(w + 1) * LANES]
        copy_to(parts.at[h, 1 - half], paired.at[h], partner, col, image_sem.at[0, h], image_sem.at[1, h])

    for h in range(2):
        wait_for(paired.at[h], image_sem.at[1, h])
        sums[h] = parts[h, half] + paired[h]

        def scatter(k, carry):
            there_row, there_col = target(k)
            copy_to(sums.at[h, there_row * cols + there_col], shares.at[h, seat], there_row * 2 + half, there_col, image_sem.at[2, h], image_sem.at[3, h])
            return carry

        lax.fori_loop(0, members - 1, scatter, 0)
        shares[h, seat] = sums[h, seat]

    for h in range(2):
        wait_for(shares.at[h, pl.ds(0, members - 1)], image_sem.at[3, h])
        mine[h] = jnp.sum(shares[h], axis=0)

        def gather(k, carry):
            there_row, there_col = target(k)
            copy_to(mine.at[h], spread.at[h, half, seat], there_row * 2 + half, there_col, image_sem.at[4, h], image_sem.at[5, h])
            return carry

        lax.fori_loop(0, members - 1, gather, 0)
        spread[h, half, seat] = mine[h]

    for h in range(2):
        wait_for(spread.at[h, half, pl.ds(0, members - 1)], image_sem.at[5, h])
        copy_to(spread.at[h, half], spread.at[h, half], partner, col, image_sem.at[6, h], image_sem.at[7, h])

    images = []
    for h in range(2):
        wait_for(spread.at[h, half], image_sem.at[7, h])
        images.append(jnp.concatenate([
            jnp.concatenate([spread[h, i // members, i % members, j] for i in range(r * spans, (r + 1) * spans) for j in range(each)], axis=1)
            for r in range(half_rank // 8)], axis=0))
        deal(left_split(images[h], hat_high[...], hat_low[...]), deals.at[1, h])
        send_deal(1, h)

    image = jnp.concatenate(images, axis=0)
    lower = dot(image, image, ((1,), (1,)))
    shape = lower.shape
    lower, inverse = eliminate(lower, ones_where(iota(shape, 0) == iota(shape, 1)), 0, rank_one // 3)
    store_lanes(whole_two, rank_four, lane_high, lane_low)
    left = expand_rows(whole_three.T, copies)
    wait_deal(1)
    contract(1, left)
    send_back(1)
    lower, inverse = eliminate(lower, inverse, rank_one // 3, rank_one)
    basis_ref[...] = dot(inverse, image, ((1,), (0,)))
    wait_back(1, 0)
    wait_back(1, 1)
    core = dot(jnp.concatenate([collect(1, 0), collect(1, 1)], axis=0), inverse, ((0,), (1,)))
    for c in range(local_three):
        for b in range(local_two):
            core_ref[b, c] = core[(c * local_two + b) * rank_four:(c * local_two + b + 1) * rank_four, :]

    for stage in range(2):
        wait_for(dealt.at[stage, pl.ds(0, (devices - 1) * tile)], send_sem.at[stage])
        wait_for(dealt.at[stage, pl.ds(0, (devices - 1) * tile)], send_sem.at[2 + stage])
    for h in range(2):
        wait_for(paired.at[h], image_sem.at[0, h])
        wait_for(shares.at[h, pl.ds(0, members - 1)], image_sem.at[2, h])
        wait_for(shares.at[h, pl.ds(0, members - 1)], image_sem.at[4, h])
        wait_for(paired.at[h], image_sem.at[6, h])
    wait_for(twos.at[pl.ds(0, rows - 1)], factor_sem.at[0])
    wait_for(threes.at[pl.ds(0, cols - 1)], factor_sem.at[2])


def write_kernel(core_ref, basis_ref, core_hbm, basis_hbm, sem):
    first = pltpu.make_async_copy(core_ref, core_hbm, sem.at[0])
    second = pltpu.make_async_copy(basis_ref, basis_hbm, sem.at[1])
    first.start()
    second.start()
    first.wait()
    second.wait()


def fits(tensor, factor_two, factor_three, factor_four, factor_init):
    rows, cols = lax.axis_size("row"), lax.axis_size("col")
    devices = rows * cols
    first_len, local_two, width = tensor.shape
    fourth_len, rank_four = factor_four.shape
    rank_one = factor_init.shape[1]
    local_three = width // fourth_len
    same = factor_two.shape[1] == local_two * rows and factor_three.shape[1] == local_three * cols
    even = rows % 2 == 0 and cols % 2 == 0 and rank_one % 16 == 0 and rank_one % devices == 0
    flat = local_two * rank_four == LANES and width == LANES and local_three * (rank_one // devices) == 8
    tiles = (rank_one // 16) * (first_len // LANES)
    return same and even and flat and first_len % (4 * LANES) == 0 and tiles % devices == 0 and (first_len // LANES) % (tiles // devices) == 0


def fused(tensor, factor_two, factor_three, factor_four, factor_init):
    rows, cols = lax.axis_size("row"), lax.axis_size("col")
    devices = rows * cols
    members = devices // 2
    first_len, local_two, width = tensor.shape
    fourth_len, rank_four = factor_four.shape
    rank_one = factor_init.shape[1]
    local_three = width // fourth_len
    lanes = local_two * rank_four
    features = local_three * lanes
    total_width = local_two * width
    tile = local_three * (rank_one // devices)
    each = (rank_one // 16) * (first_len // LANES) // devices
    wide = rows * lanes

    def f32(*shape):
        return pltpu.VMEM(shape, jnp.float32)

    def bf16(*shape):
        return pltpu.VMEM(shape, jnp.bfloat16)

    vmem, hbm = pl.BlockSpec(memory_space=pltpu.VMEM), pl.BlockSpec(memory_space=pltpu.HBM)
    shapes = (
        jax.ShapeDtypeStruct((local_two, local_three, rank_four, rank_one), jnp.float32),
        jax.ShapeDtypeStruct((rank_one, first_len), jnp.float32),
    )
    operands = [pltpu.with_memory_space_constraint(x, pltpu.HBM) for x in (tensor, factor_two, factor_three, factor_four.T, factor_init.T)]
    core, basis = pl.pallas_call(
        hooi_kernel,
        out_shape=tuple(pltpu.VMEM(x.shape, x.dtype) for x in shapes),
        in_specs=[hbm] * 5,
        out_specs=(vmem, vmem),
        scratch_shapes=[
            f32(local_two, first_len, width), f32(*factor_two.shape), f32(*factor_three.shape), f32(rank_four, fourth_len), f32(rank_one, first_len),
            bf16(first_len, total_width), bf16(first_len, total_width), bf16(total_width, features), bf16(total_width, features),
            bf16(first_len, features), bf16(first_len, features), bf16(features, first_len), bf16(features, first_len),
            bf16(wide, wide), bf16(wide, wide), f32(rows, *factor_two.shape), f32(cols, *factor_three.shape),
            f32(2, 2, members * tile, lanes), f32(2, devices * tile, lanes), f32(2, devices * tile, lanes), f32(2, 2, members * tile, lanes),
            f32(2, 2, members, each, 8, LANES), f32(2, members, each, 8, LANES), f32(2, members, each, 8, LANES), f32(2, members, each, 8, LANES),
            f32(2, each, 8, LANES), f32(2, 2, members, each, 8, LANES),
            pltpu.SemaphoreType.DMA((local_two + 4,)),
            pltpu.SemaphoreType.DMA((4,)),
            pltpu.SemaphoreType.DMA((4,)),
            pltpu.SemaphoreType.DMA((2,)),
            pltpu.SemaphoreType.DMA((2, 2)),
            pltpu.SemaphoreType.DMA((8, 2)),
        ],
        compiler_params=pltpu.CompilerParams(collective_id=0, has_side_effects=True, vmem_limit_bytes=48 << 20),
    )(*operands)
    core, basis = pl.pallas_call(
        write_kernel,
        out_shape=shapes,
        in_specs=[vmem, vmem],
        out_specs=(hbm, hbm),
        scratch_shapes=[pltpu.SemaphoreType.DMA((2,))],
        compiler_params=pltpu.CompilerParams(vmem_limit_bytes=4 << 20),
    )(core, basis)
    return basis.T, core.transpose(3, 0, 1, 2)


def shards(tensor, factor_two, factor_three, factor_four, factor_init):
    if fits(tensor, factor_two, factor_three, factor_four, factor_init):
        return fused(tensor, factor_two, factor_three, factor_four, factor_init)
    axes = ("row", "col")
    first_len, local_two, width = tensor.shape
    fourth_len, rank_four = factor_four.shape
    local_three = width // fourth_len
    rank_one = factor_init.shape[1]
    rows, cols = lax.axis_size("row"), lax.axis_size("col")
    devices = rows * cols
    local_pairs = local_two * local_three
    features = rank_four * rank_one
    part = features // devices
    data = tensor.reshape(first_len, local_pairs, fourth_len)
    rank_two, rank_three = factor_two.shape[1], factor_three.shape[1]

    def pull(vectors):
        mixed = jnp.einsum("apd,ar->prd", data, vectors, precision=lax.Precision.HIGH)
        return jnp.einsum("prd,de->per", mixed, factor_four, precision=HIGHEST).reshape(local_pairs, features)

    def share(values, ident):
        length = values.shape[1]
        padded = -(-length // LANES) * LANES
        values = jnp.pad(values, ((0, 0), (0, padded - length))).reshape(devices, padded // LANES, LANES)
        return swap(values, ident).reshape(devices, padded)[:, :length]

    def spread(block, ident, extra=None):
        put = block.reshape(local_pairs, devices, part).transpose(1, 0, 2).reshape(devices, local_pairs * part)
        if extra is not None:
            put = jnp.concatenate([put, jnp.broadcast_to(extra[None], (devices, extra.shape[0]))], axis=1)
        got = share(put, ident)
        rest = got[:, local_pairs * part:]
        got = got[:, :local_pairs * part]
        got = got.reshape(rows, cols, local_two, local_three, part)
        return got.transpose(0, 2, 1, 3, 4).reshape(rows * local_two, cols * local_three, part), rest

    def gather(block, ident):
        two, three, _ = block.shape
        put = block.reshape(rows, two // rows, cols, three // cols, part).transpose(0, 2, 1, 3, 4)
        got = share(put.reshape(devices, -1), ident).reshape(devices, (two // rows) * (three // cols), part)
        return got.transpose(1, 0, 2).reshape(got.shape[1], features)

    extra = jnp.concatenate([factor_two.reshape(-1), factor_three.reshape(-1)])
    block, rest = spread(pull(factor_init), 1, extra)
    rest = rest.reshape(rows, cols, -1)
    whole_two = rest[:, 0, :factor_two.size].reshape(-1, rank_two)
    whole_three = rest[0, :, factor_two.size:].reshape(-1, rank_three)
    block = jnp.einsum("bcq,bg->gcq", block, whole_two, precision=HIGHEST)
    block = jnp.einsum("gcq,cf->gfq", block, whole_three, precision=HIGHEST)
    block = jnp.einsum("gfq,cf->gcq", block, whole_three, precision=HIGHEST)
    block = jnp.einsum("gcq,bg->bcq", block, whole_two, precision=HIGHEST)
    block = gather(block, 2).reshape(local_pairs, rank_four, rank_one)
    block = jnp.einsum("per,de->pdr", block, factor_four, precision=HIGHEST)
    image = jnp.dot(tensor.reshape(first_len, -1), block.reshape(-1, rank_one), precision=lax.Precision.HIGH)
    half = first_len // 2
    image = jnp.concatenate([image[:half], image[half:]], axis=1).reshape(devices, half // devices, 2 * rank_one)
    image = total(image, 0).reshape(half, 2 * rank_one)
    image = jnp.concatenate([image[:, :rank_one], image[:, rank_one:]], axis=0)
    basis, inverse = finish(image)
    block, _ = spread(pull(image), 3)
    block = jnp.einsum("bcq,bg->gcq", block, whole_two, precision=HIGHEST)
    block = jnp.einsum("gcq,cf->gfq", block, whole_three, precision=HIGHEST)
    block = gather(block, 4).reshape(-1, rank_four, rank_one)
    core = jnp.einsum("per,sr->spe", block, inverse, precision=HIGHEST)
    return (basis, core.reshape(rank_one, rank_two // rows, rank_three // cols, rank_four))


def solution(mesh):
    in_specs = (P(None, "row", "col"), P("row", None), P("col", None), P(), P())
    out_specs = (P(), P(None, "row", "col", None))
    return jax.shard_map(shards, mesh=mesh, in_specs=in_specs, out_specs=out_specs, check_vma=False)
```

```python
import functools

import jax
import jax.numpy as jnp
from jax import lax
from jax.experimental import pallas as pl
from jax.experimental.pallas import tpu as pltpu
from jax.sharding import PartitionSpec as P

HIGHEST = lax.Precision.HIGHEST
LANES = 128


def dot(a, b, dims):
    return lax.dot_general(a, b, (dims, ((), ())), precision=HIGHEST, preferred_element_type=jnp.float32)


def inverse_factor(square):
    size = square.shape[0]
    rows = lax.broadcasted_iota(jnp.int32, (size, size), 0)
    cols = lax.broadcasted_iota(jnp.int32, (size, size), 1)
    index = lax.broadcasted_iota(jnp.int32, (size, 1), 0)
    left = square
    right = jnp.where(rows == cols, 1.0, 0.0).astype(jnp.float32)
    for k in range(size):
        scale = lax.rsqrt(left[k:k + 1, k:k + 1])
        column = left[:, k:k + 1] * scale
        pivot_left = left[k:k + 1, :] * scale
        pivot_right = right[k:k + 1, :] * scale
        factor = jnp.where(index > k, column, 0.0)
        left = left - factor * pivot_left
        right = jnp.where(index == k, pivot_right, right - factor * pivot_right)
    return right


def finish_kernel(image_ref, basis_ref, inverse_ref):
    image = image_ref[...]
    inverse = inverse_factor(dot(image, image, ((0,), (0,))))
    inverse_ref[...] = inverse
    basis_ref[...] = dot(image, inverse, ((1,), (1,)))


def finish(image):
    rank = image.shape[1]
    return pl.pallas_call(
        finish_kernel,
        out_shape=(
            jax.ShapeDtypeStruct(image.shape, jnp.float32),
            jax.ShapeDtypeStruct((rank, rank), jnp.float32),
        ),
    )(image)


def place():
    return lax.axis_index("row") * lax.axis_size("col") + lax.axis_index("col")


def greet(devices):
    cols = lax.axis_size("col")
    me = place()
    barrier = pltpu.get_barrier_semaphore()

    def hello(k, carry):
        peer = lax.rem(me + k, devices)
        pl.semaphore_signal(barrier, inc=1, device_id=(peer // cols, lax.rem(peer, cols)), device_id_type=pl.DeviceIdType.MESH)
        return carry

    lax.fori_loop(1, devices, hello, 0)
    pl.semaphore_wait(barrier, devices - 1)


def send_all(devices, source, target, send_sem, recv_sem):
    cols = lax.axis_size("col")
    me = place()

    def send(k, carry):
        peer = lax.rem(me + k, devices)
        pltpu.make_async_remote_copy(
            src_ref=source(peer),
            dst_ref=target.at[me],
            send_sem=send_sem,
            recv_sem=recv_sem,
            device_id=(peer // cols, lax.rem(peer, cols)),
            device_id_type=pl.DeviceIdType.MESH,
        ).start()
        return carry

    lax.fori_loop(1, devices, send, 0)
    whole = target.at[pl.ds(0, devices - 1)]
    pltpu.make_async_copy(whole, whole, send_sem).wait()
    pltpu.make_async_copy(whole, whole, recv_sem).wait()


def swap_kernel(devices, put_ref, out_ref, held, send_sem, recv_sem):
    me = place()
    greet(devices)
    send_all(devices, lambda peer: put_ref.at[peer], held, send_sem, recv_sem)
    held[me] = put_ref[me]
    out_ref[...] = held[...]


def total_kernel(devices, put_ref, out_ref, held, mine, spread, sems):
    me = place()
    greet(devices)
    send_all(devices, lambda peer: put_ref.at[peer], held, sems.at[0], sems.at[1])
    held[me] = put_ref[me]
    mine[...] = jnp.sum(held[...], axis=0)
    send_all(devices, lambda peer: mine, spread, sems.at[2], sems.at[3])
    spread[me] = mine[...]
    out_ref[...] = spread[...]


def swap(values, ident):
    devices = values.shape[0]
    return pl.pallas_call(
        functools.partial(swap_kernel, devices),
        out_shape=jax.ShapeDtypeStruct(values.shape, jnp.float32),
        in_specs=[pl.BlockSpec(memory_space=pltpu.VMEM)],
        out_specs=pl.BlockSpec(memory_space=pltpu.VMEM),
        scratch_shapes=[pltpu.VMEM(values.shape, jnp.float32), pltpu.SemaphoreType.DMA, pltpu.SemaphoreType.DMA],
        compiler_params=pltpu.CompilerParams(collective_id=ident, has_side_effects=True),
    )(values)


def total(values, ident):
    devices = values.shape[0]
    return pl.pallas_call(
        functools.partial(total_kernel, devices),
        out_shape=jax.ShapeDtypeStruct(values.shape, jnp.float32),
        in_specs=[pl.BlockSpec(memory_space=pltpu.VMEM)],
        out_specs=pl.BlockSpec(memory_space=pltpu.VMEM),
        scratch_shapes=[
            pltpu.VMEM(values.shape, jnp.float32),
            pltpu.VMEM(values.shape[1:], jnp.float32),
            pltpu.VMEM(values.shape, jnp.float32),
            pltpu.SemaphoreType.DMA((4,)),
        ],
        compiler_params=pltpu.CompilerParams(collective_id=ident, has_side_effects=True),
    )(values)


def split(x):
    high = x.astype(jnp.bfloat16)
    return high, (x - high.astype(jnp.float32)).astype(jnp.bfloat16)


def narrow(a, b):
    return lax.dot_general(a, b, (((1,), (0,)), ((), ())), preferred_element_type=jnp.float32)


def left_split(x, high, low):
    rows = x.shape[0]
    top, rest = split(x)
    both = narrow(jnp.concatenate([top, rest], axis=0), high)
    return both[:rows] + both[rows:] + narrow(top, low)


def iota(shape, dim):
    return lax.broadcasted_iota(jnp.int32, shape, dim)


def ones_where(mask):
    return jnp.where(mask, 1.0, 0.0).astype(jnp.float32)


def expand_rows(square, copies):
    tall = (square.shape[0] * copies, square.shape[0])
    wide = (square.shape[1], square.shape[1] * copies)
    result = dot(ones_where(iota(tall, 0) // copies == iota(tall, 1)), square, ((1,), (0,)))
    result = dot(result, ones_where(iota(wide, 1) // copies == iota(wide, 0)), ((1,), (0,)))
    return jnp.where(iota(result.shape, 0) % copies == iota(result.shape, 1) % copies, result, 0.0)


def store_lanes(matrix, copies, high_ref, low_ref):
    shape = (matrix.shape[1], matrix.shape[1] * copies)
    wide = dot(matrix, ones_where(iota(shape, 1) // copies == iota(shape, 0)), ((1,), (0,)))
    shape = (copies, shape[1])
    keep = iota(shape, 1) % copies == iota(shape, 0)
    for k in range(matrix.shape[0]):
        high, low = split(jnp.where(keep, jnp.broadcast_to(wide[k:k + 1, :], shape), 0.0))
        high_ref[k * copies:(k + 1) * copies, :] = high
        low_ref[k * copies:(k + 1) * copies, :] = low


def eliminate(left, right, first, last):
    size = left.shape[0]
    index = iota((size, 1), 0)
    for k in range(first, last):
        scale = lax.rsqrt(left[k:k + 1, k:k + 1])
        column = left[:, k:k + 1] * scale
        pivot_left = left[k:k + 1, :] * scale
        pivot_right = right[k:k + 1, :] * scale
        factor = jnp.where(index > k, column, 0.0)
        left = left - factor * pivot_left
        right = jnp.where(index == k, pivot_right, right - factor * pivot_right)
    return left, right


def copy_to(source, target, row, col, send_sem, recv_sem):
    pltpu.make_async_remote_copy(
        src_ref=source,
        dst_ref=target,
        send_sem=send_sem,
        recv_sem=recv_sem,
        device_id=(row, col),
        device_id_type=pl.DeviceIdType.MESH,
    ).start()


def wait_for(ref, sem):
    pltpu.make_async_copy(ref, ref, sem).wait()


def hooi_kernel(tensor_hbm, two_hbm, three_hbm, four_hbm, init_hbm, core_ref, basis_ref,
                slabs, two_ref, three_ref, four_ref, init_ref,
                high_ref, low_ref, mix_high, mix_low, hat_high, hat_low, turn_high, turn_low,
                lane_high, lane_low, twos, threes, puts, gots,
                parts, paired, sums, shares, mine, spread,
                load_sem, factor_sem, send_sem, recv_sem, image_sem, share_sem):
    rows, cols = lax.axis_size("row"), lax.axis_size("col")
    row, col = lax.axis_index("row"), lax.axis_index("col")
    devices = rows * cols
    members = devices // 2
    half = lax.rem(row, 2)
    seat = (row // 2) * cols + col
    me = row * cols + col
    partner = row + 1 - 2 * half
    rank_one, first_len = init_ref.shape
    half_len = first_len // 2
    local_two, local_three = two_ref.shape[0], three_ref.shape[0]
    rank_four, fourth_len = four_ref.shape
    width = local_three * fourth_len
    lanes = local_two * rank_four
    features = local_three * lanes
    copies = rank_one // devices
    tile = local_three * copies
    each = sums.shape[0]
    spans = half_len // LANES

    slab_loads = [pltpu.make_async_copy(tensor_hbm.at[:, b, :], slabs.at[b], load_sem.at[b]) for b in range(local_two)]
    small = [(four_hbm, four_ref), (init_hbm, init_ref), (two_hbm, two_ref), (three_hbm, three_ref)]
    small_loads = [pltpu.make_async_copy(source, target, load_sem.at[local_two + k]) for k, (source, target) in enumerate(small)]
    small_loads[0].start()
    small_loads[1].start()
    for load in slab_loads:
        load.start()
    small_loads[2].start()
    small_loads[3].start()

    def target(k):
        turn = k // (rows // 2)
        shift = (turn + 1) // 2
        there = lax.rem(col + cols // 2 + cols + (1 - 2 * lax.rem(turn, 2)) * shift, cols)
        return lax.rem(row // 2 + rows - 1 - lax.rem(k, rows // 2), rows // 2), there

    def at(index, count):
        return pl.ds(pl.multiple_of(index * count, count), count)

    barrier = pltpu.get_barrier_semaphore()

    def greet_at(there_row, there_col):
        pl.semaphore_signal(barrier, inc=1, device_id=(there_row, there_col), device_id_type=pl.DeviceIdType.MESH)

    def hello(k, carry):
        there_row, there_col = target(members - 1 - rows // 2 - k)
        greet_at(there_row * 2, there_col)
        greet_at(there_row * 2 + 1, there_col)
        return carry

    def hello_near(k, carry):
        greet_at(lax.rem(row + k, rows), col)
        return carry

    lax.fori_loop(0, members - rows // 2, hello, 0)
    lax.fori_loop(1, rows, hello_near, 0)

    small_loads[0].wait()
    lane = iota((fourth_len, features), 1)
    shape = (rank_four, features)
    four = dot(four_ref[...], ones_where(iota(shape, 1) % rank_four == iota(shape, 0)), ((0,), (0,)))
    four_high = four.astype(jnp.bfloat16).astype(jnp.float32)
    four_low = four - four_high
    for b in range(local_two):
        for c in range(local_three):
            keep = lane // rank_four == c * local_two + b
            part = slice((b * local_three + c) * fourth_len, (b * local_three + c + 1) * fourth_len)
            mix_high[part, :] = jnp.where(keep, four_high, 0.0).astype(jnp.bfloat16)
            mix_low[part, :] = jnp.where(keep, four_low, 0.0).astype(jnp.bfloat16)

    small_loads[1].wait()
    init_high, init_low = split(init_ref[...])
    init_both = jnp.concatenate([init_high, init_low], axis=0)
    group = 4 if local_two % 4 == 0 else 1
    count = local_two // group

    def pull_group(k):
        part = slice(k * group * width, (k + 1) * group * width)
        both = narrow(init_both, high_ref[:, part])
        return both[:rank_one] + both[rank_one:] + narrow(init_high, low_ref[:, part])

    def mix_group(k, pulled):
        part = slice(k * group * width, (k + 1) * group * width)
        return left_split(pulled, mix_high[part, :], mix_low[part, :])

    pulled, vectors = [], []
    for k in range(count + 2):
        if k < count:
            for b in range(k * group, (k + 1) * group):
                slab_loads[b].wait()
                high, low = split(slabs[b])
                high_ref[:, b * width:(b + 1) * width] = high
                low_ref[:, b * width:(b + 1) * width] = low
        if k >= 2:
            vectors.append(mix_group(k - 2, pulled[k - 2]))
        if 1 <= k <= count:
            pulled.append(pull_group(k - 1))
    vectors = sum(vectors[1:], vectors[0])

    def deal(vectors, put):
        for c in range(local_three):
            for k in range(copies):
                put[pl.ds(c * copies + k, devices, stride=tile), :] = vectors[k * devices:(k + 1) * devices, c * lanes:(c + 1) * lanes]

    def send(stage):
        put, got = puts.at[stage], gots.at[stage]

        def one(there_row, there_col):
            copy_to(put.at[at(there_row * cols + there_col, tile)], got.at[at(me, tile)], there_row, there_col, send_sem.at[stage], recv_sem.at[stage])

        def some(k, carry):
            there_row, there_col = target(lax.rem(k, members - 1))
            one(there_row * 2 + k // (members - 1), there_col)
            return carry

        def both(k, carry):
            there_row, there_col = target(k)
            one(there_row * 2, there_col)
            one(there_row * 2 + 1, there_col)
            return carry

        if stage in (0, 1, 2, 3):
            lax.fori_loop(0, 2 * (members - 1), some, 0, unroll=5 if (members - 1) % 5 == 0 else 1)
        else:
            lax.fori_loop(0, members - 1, both, 0, unroll=3 if (members - 1) % 3 == 0 else 1)
        one(partner, col)
        here = at(me, tile)
        got[here, :] = put[here, :]

    def arrive(stage):
        wait_for(gots.at[stage, pl.ds(0, (devices - 1) * tile)], recv_sem.at[stage])

    def contract(stage, matrix):
        block = jnp.concatenate([gots[stage, k * cols * tile:(k + 1) * cols * tile, :] for k in range(rows)], axis=1)
        top, rest = split(block)
        result = left_split(narrow(matrix, jnp.concatenate([top, top, rest], axis=0)), lane_high[...], lane_low[...])
        for k in range(rows):
            puts[stage + 1, k * cols * tile:(k + 1) * cols * tile, :] = result[:, k * lanes:(k + 1) * lanes]

    def triple(matrix, axis):
        high, low = split(matrix)
        return jnp.concatenate([high, low, high], axis=axis)

    def collect(stage):
        got = gots.at[stage]
        return jnp.concatenate([
            jnp.concatenate([got[pl.ds(c * copies + k, devices, stride=tile), :] for k in range(copies)], axis=0)
            for c in range(local_three)], axis=1)

    deal(vectors, puts.at[0])
    small_loads[2].wait()
    small_loads[3].wait()
    pl.semaphore_wait(barrier, devices - 1)

    def send_two(k, carry):
        copy_to(two_ref, twos.at[row], lax.rem(row + k, rows), col, factor_sem.at[0], factor_sem.at[1])
        return carry

    def send_three(k, carry):
        copy_to(three_ref, threes.at[col], row, lax.rem(col + k, cols), factor_sem.at[2], factor_sem.at[3])
        return carry

    lax.fori_loop(1, rows, send_two, 0)
    lax.fori_loop(1, cols, send_three, 0)
    send(0)
    twos[row] = two_ref[...]
    threes[col] = three_ref[...]

    def hat_piece(k, count):
        part = slice(k * first_len // count, (k + 1) * first_len // count)
        hat = narrow(high_ref[part, :], mix_high[...]) + narrow(high_ref[part, :], mix_low[...]) + narrow(low_ref[part, :], mix_high[...])
        hat_high[part, :], hat_low[part, :] = split(hat)
        turn_high[:, part], turn_low[:, part] = split(hat.T)

    hat_piece(0, 4)
    hat_piece(1, 4)
    wait_for(twos.at[pl.ds(0, rows - 1)], factor_sem.at[1])
    wait_for(threes.at[pl.ds(0, cols - 1)], factor_sem.at[3])
    whole_two = jnp.concatenate([twos[k] for k in range(rows)], axis=0)
    whole_three = jnp.concatenate([threes[k] for k in range(cols)], axis=0)
    store_lanes(dot(whole_two, whole_two, ((1,), (1,))), rank_four, lane_high, lane_low)
    left = triple(expand_rows(dot(whole_three, whole_three, ((1,), (1,))), copies), 1)

    arrive(0)
    contract(0, left)
    send(1)
    hat_piece(2, 4)
    hat_piece(3, 4)

    arrive(1)
    back = collect(1)

    def image_part(which):
        span = at(which, half_len)
        return left_split(back, turn_high[:, span], turn_low[:, span])

    def tiles():
        for i in range(members):
            for j in range(each):
                r, w = (i * each + j) // spans, (i * each + j) % spans
                yield i, j, slice(r * 8, (r + 1) * 8), slice(w * LANES, (w + 1) * LANES)

    image = image_part(1 - half)
    for i, j, r, w in tiles():
        parts[j, i] = image[r, w]
    copy_to(parts, paired, partner, col, image_sem.at[0], image_sem.at[1])
    image = image_part(half)
    wait_for(paired, image_sem.at[1])
    for i, j, r, w in tiles():
        sums[j, i] = image[r, w] + paired[j, i]

    for j in range(each):
        def scatter(k, carry):
            there_row, there_col = target(k)
            copy_to(sums.at[j, there_row * cols + there_col], shares.at[j, seat], there_row * 2 + 1 - half, there_col, share_sem.at[0, j], share_sem.at[1, j])
            return carry

        lax.fori_loop(0, members, scatter, 0, unroll=4)
    for j in range(each):
        wait_for(shares.at[j], share_sem.at[1, j])
        mine[j] = jnp.sum(shares[j], axis=0)

        def gather(k, carry):
            there_row, there_col = target(k)
            copy_to(mine.at[j], spread.at[1 - half, j, seat], there_row * 2 + 1 - half, there_col, share_sem.at[2, j], share_sem.at[3, j])
            return carry

        lax.fori_loop(0, members, gather, 0, unroll=4)
    for j in range(each):
        wait_for(spread.at[half, j], share_sem.at[3, j])
        copy_to(spread.at[half, j], spread.at[half, j], partner, col, image_sem.at[2], image_sem.at[3])

    def image_half(which):
        return jnp.concatenate([
            jnp.concatenate([spread[which, (r * spans + w) % each, (r * spans + w) // each] for w in range(spans)], axis=1)
            for r in range(rank_one // 8)], axis=0)

    def pull_half(which):
        span = at(which, half_len)
        return left_split(image_half(which), hat_high[span, :], hat_low[span, :])

    vectors = pull_half(half)
    wait_for(spread.at[1 - half], image_sem.at[3])
    deal(vectors + pull_half(1 - half), puts.at[2])
    send(2)

    image = jnp.concatenate([image_half(0), image_half(1)], axis=1)
    lower = dot(image, image, ((1,), (1,)))
    shape = lower.shape
    lower, inverse = eliminate(lower, ones_where(iota(shape, 0) == iota(shape, 1)), 0, rank_one * 5 // 8)
    store_lanes(whole_two, rank_four, lane_high, lane_low)
    left = triple(expand_rows(whole_three.T, copies), 1)
    arrive(2)
    contract(2, left)
    send(3)
    lower, inverse = eliminate(lower, inverse, rank_one * 5 // 8, rank_one)
    basis_ref[...] = dot(inverse, image, ((1,), (0,)))
    inverse_high, inverse_low = split(inverse.T)
    weights = jnp.concatenate([inverse_high, inverse_high, inverse_low], axis=0)
    arrive(3)
    core = lax.dot_general(triple(collect(3), 0), weights, (((0,), (0,)), ((), ())), preferred_element_type=jnp.float32)
    for c in range(local_three):
        for b in range(local_two):
            core_ref[b, c] = core[(c * local_two + b) * rank_four:(c * local_two + b + 1) * rank_four, :]

    for stage in range(4):
        wait_for(gots.at[stage, pl.ds(0, (devices - 1) * tile)], send_sem.at[stage])
    wait_for(paired, image_sem.at[0])
    wait_for(paired, image_sem.at[2])
    for j in range(each):
        wait_for(shares.at[j], share_sem.at[0, j])
        wait_for(shares.at[j], share_sem.at[2, j])
    wait_for(twos.at[pl.ds(0, rows - 1)], factor_sem.at[0])
    wait_for(threes.at[pl.ds(0, cols - 1)], factor_sem.at[2])


def write_kernel(core_ref, basis_ref, core_hbm, basis_hbm, sem):
    first = pltpu.make_async_copy(core_ref, core_hbm, sem.at[0])
    second = pltpu.make_async_copy(basis_ref, basis_hbm, sem.at[1])
    first.start()
    second.start()
    first.wait()
    second.wait()


def fits(tensor, factor_two, factor_three, factor_four, factor_init):
    rows, cols = lax.axis_size("row"), lax.axis_size("col")
    devices = rows * cols
    first_len, local_two, width = tensor.shape
    fourth_len, rank_four = factor_four.shape
    rank_one = factor_init.shape[1]
    local_three = width // fourth_len
    same = factor_two.shape[1] == local_two * rows and factor_three.shape[1] == local_three * cols
    even = rows % 2 == 0 and cols % 2 == 0 and rank_one % devices == 0
    flat = local_two * rank_four == LANES and width == LANES and local_three * (rank_one // devices) == 8
    tiles = (rank_one // 8) * (first_len // LANES)
    return same and even and flat and first_len % (4 * LANES) == 0 and tiles % devices == 0


def fused(tensor, factor_two, factor_three, factor_four, factor_init):
    rows, cols = lax.axis_size("row"), lax.axis_size("col")
    devices = rows * cols
    members = devices // 2
    first_len, local_two, width = tensor.shape
    fourth_len, rank_four = factor_four.shape
    rank_one = factor_init.shape[1]
    local_three = width // fourth_len
    lanes = local_two * rank_four
    features = local_three * lanes
    total_width = local_two * width
    tile = local_three * (rank_one // devices)
    each = (rank_one // 8) * (first_len // LANES) // devices
    wide = rows * lanes

    def f32(*shape):
        return pltpu.VMEM(shape, jnp.float32)

    def bf16(*shape):
        return pltpu.VMEM(shape, jnp.bfloat16)

    vmem, hbm = pl.BlockSpec(memory_space=pltpu.VMEM), pl.BlockSpec(memory_space=pltpu.HBM)
    shapes = (
        jax.ShapeDtypeStruct((local_two, local_three, rank_four, rank_one), jnp.float32),
        jax.ShapeDtypeStruct((rank_one, first_len), jnp.float32),
    )
    operands = [pltpu.with_memory_space_constraint(x, pltpu.HBM) for x in (tensor, factor_two, factor_three, factor_four.T, factor_init.T)]
    core, basis = pl.pallas_call(
        hooi_kernel,
        out_shape=tuple(pltpu.VMEM(x.shape, x.dtype) for x in shapes),
        in_specs=[hbm] * 5,
        out_specs=(vmem, vmem),
        scratch_shapes=[
            f32(local_two, first_len, width), f32(*factor_two.shape), f32(*factor_three.shape), f32(rank_four, fourth_len), f32(rank_one, first_len),
            bf16(first_len, total_width), bf16(first_len, total_width), bf16(total_width, features), bf16(total_width, features),
            bf16(first_len, features), bf16(first_len, features), bf16(features, first_len), bf16(features, first_len),
            bf16(wide, wide), bf16(wide, wide), f32(rows, *factor_two.shape), f32(cols, *factor_three.shape),
            f32(4, devices * tile, lanes), f32(4, devices * tile, lanes),
            f32(each, members, 8, LANES), f32(each, members, 8, LANES), f32(each, members, 8, LANES), f32(each, members, 8, LANES),
            f32(each, 8, LANES), f32(2, each, members, 8, LANES),
            pltpu.SemaphoreType.DMA((local_two + 4,)),
            pltpu.SemaphoreType.DMA((4,)),
            pltpu.SemaphoreType.DMA((4,)),
            pltpu.SemaphoreType.DMA((4,)),
            pltpu.SemaphoreType.DMA((4,)),
            pltpu.SemaphoreType.DMA((4, each)),
        ],
        compiler_params=pltpu.CompilerParams(collective_id=0, has_side_effects=True, vmem_limit_bytes=48 << 20),
    )(*operands)
    core, basis = pl.pallas_call(
        write_kernel,
        out_shape=shapes,
        in_specs=[vmem, vmem],
        out_specs=(hbm, hbm),
        scratch_shapes=[pltpu.SemaphoreType.DMA((2,))],
        compiler_params=pltpu.CompilerParams(vmem_limit_bytes=4 << 20),
    )(core, basis)
    return basis.T, core.transpose(3, 0, 1, 2)


def shards(tensor, factor_two, factor_three, factor_four, factor_init):
    if fits(tensor, factor_two, factor_three, factor_four, factor_init):
        return fused(tensor, factor_two, factor_three, factor_four, factor_init)
    axes = ("row", "col")
    first_len, local_two, width = tensor.shape
    fourth_len, rank_four = factor_four.shape
    local_three = width // fourth_len
    rank_one = factor_init.shape[1]
    rows, cols = lax.axis_size("row"), lax.axis_size("col")
    devices = rows * cols
    local_pairs = local_two * local_three
    features = rank_four * rank_one
    part = features // devices
    data = tensor.reshape(first_len, local_pairs, fourth_len)
    rank_two, rank_three = factor_two.shape[1], factor_three.shape[1]

    def pull(vectors):
        mixed = jnp.einsum("apd,ar->prd", data, vectors, precision=lax.Precision.HIGH)
        return jnp.einsum("prd,de->per", mixed, factor_four, precision=HIGHEST).reshape(local_pairs, features)

    def share(values, ident):
        length = values.shape[1]
        padded = -(-length // LANES) * LANES
        values = jnp.pad(values, ((0, 0), (0, padded - length))).reshape(devices, padded // LANES, LANES)
        return swap(values, ident).reshape(devices, padded)[:, :length]

    def spread(block, ident, extra=None):
        put = block.reshape(local_pairs, devices, part).transpose(1, 0, 2).reshape(devices, local_pairs * part)
        if extra is not None:
            put = jnp.concatenate([put, jnp.broadcast_to(extra[None], (devices, extra.shape[0]))], axis=1)
        got = share(put, ident)
        rest = got[:, local_pairs * part:]
        got = got[:, :local_pairs * part]
        got = got.reshape(rows, cols, local_two, local_three, part)
        return got.transpose(0, 2, 1, 3, 4).reshape(rows * local_two, cols * local_three, part), rest

    def gather(block, ident):
        two, three, _ = block.shape
        put = block.reshape(rows, two // rows, cols, three // cols, part).transpose(0, 2, 1, 3, 4)
        got = share(put.reshape(devices, -1), ident).reshape(devices, (two // rows) * (three // cols), part)
        return got.transpose(1, 0, 2).reshape(got.shape[1], features)

    extra = jnp.concatenate([factor_two.reshape(-1), factor_three.reshape(-1)])
    block, rest = spread(pull(factor_init), 1, extra)
    rest = rest.reshape(rows, cols, -1)
    whole_two = rest[:, 0, :factor_two.size].reshape(-1, rank_two)
    whole_three = rest[0, :, factor_two.size:].reshape(-1, rank_three)
    block = jnp.einsum("bcq,bg->gcq", block, whole_two, precision=HIGHEST)
    block = jnp.einsum("gcq,cf->gfq", block, whole_three, precision=HIGHEST)
    block = jnp.einsum("gfq,cf->gcq", block, whole_three, precision=HIGHEST)
    block = jnp.einsum("gcq,bg->bcq", block, whole_two, precision=HIGHEST)
    block = gather(block, 2).reshape(local_pairs, rank_four, rank_one)
    block = jnp.einsum("per,de->pdr", block, factor_four, precision=HIGHEST)
    image = jnp.dot(tensor.reshape(first_len, -1), block.reshape(-1, rank_one), precision=lax.Precision.HIGH)
    half = first_len // 2
    image = jnp.concatenate([image[:half], image[half:]], axis=1).reshape(devices, half // devices, 2 * rank_one)
    image = total(image, 0).reshape(half, 2 * rank_one)
    image = jnp.concatenate([image[:, :rank_one], image[:, rank_one:]], axis=0)
    basis, inverse = finish(image)
    block, _ = spread(pull(image), 3)
    block = jnp.einsum("bcq,bg->gcq", block, whole_two, precision=HIGHEST)
    block = jnp.einsum("gcq,cf->gfq", block, whole_three, precision=HIGHEST)
    block = gather(block, 4).reshape(-1, rank_four, rank_one)
    core = jnp.einsum("per,sr->spe", block, inverse, precision=HIGHEST)
    return (basis, core.reshape(rank_one, rank_two // rows, rank_three // cols, rank_four))


def solution(mesh):
    in_specs = (P(None, "row", "col"), P("row", None), P("col", None), P(), P())
    out_specs = (P(), P(None, "row", "col", None))
    return jax.shard_map(shards, mesh=mesh, in_specs=in_specs, out_specs=out_specs, check_vma=False)
```

```python
import functools

import jax
import jax.numpy as jnp
from jax import lax
from jax.experimental import pallas as pl
from jax.experimental.pallas import tpu as pltpu
from jax.sharding import PartitionSpec as P

HIGHEST = lax.Precision.HIGHEST
LANES = 128


def dot(a, b, dims):
    return lax.dot_general(a, b, (dims, ((), ())), precision=HIGHEST, preferred_element_type=jnp.float32)


def inverse_factor(square):
    size = square.shape[0]
    rows = lax.broadcasted_iota(jnp.int32, (size, size), 0)
    cols = lax.broadcasted_iota(jnp.int32, (size, size), 1)
    index = lax.broadcasted_iota(jnp.int32, (size, 1), 0)
    left = square
    right = jnp.where(rows == cols, 1.0, 0.0).astype(jnp.float32)
    for k in range(size):
        scale = lax.rsqrt(left[k:k + 1, k:k + 1])
        column = left[:, k:k + 1] * scale
        pivot_left = left[k:k + 1, :] * scale
        pivot_right = right[k:k + 1, :] * scale
        factor = jnp.where(index > k, column, 0.0)
        left = left - factor * pivot_left
        right = jnp.where(index == k, pivot_right, right - factor * pivot_right)
    return right


def finish_kernel(image_ref, basis_ref, inverse_ref):
    image = image_ref[...]
    inverse = inverse_factor(dot(image, image, ((0,), (0,))))
    inverse_ref[...] = inverse
    basis_ref[...] = dot(image, inverse, ((1,), (1,)))


def finish(image):
    rank = image.shape[1]
    return pl.pallas_call(
        finish_kernel,
        out_shape=(
            jax.ShapeDtypeStruct(image.shape, jnp.float32),
            jax.ShapeDtypeStruct((rank, rank), jnp.float32),
        ),
    )(image)


def place():
    return lax.axis_index("row") * lax.axis_size("col") + lax.axis_index("col")


def greet(devices):
    cols = lax.axis_size("col")
    me = place()
    barrier = pltpu.get_barrier_semaphore()

    def hello(k, carry):
        peer = lax.rem(me + k, devices)
        pl.semaphore_signal(barrier, inc=1, device_id=(peer // cols, lax.rem(peer, cols)), device_id_type=pl.DeviceIdType.MESH)
        return carry

    lax.fori_loop(1, devices, hello, 0)
    pl.semaphore_wait(barrier, devices - 1)


def send_all(devices, source, target, send_sem, recv_sem):
    cols = lax.axis_size("col")
    me = place()

    def send(k, carry):
        peer = lax.rem(me + k, devices)
        pltpu.make_async_remote_copy(
            src_ref=source(peer),
            dst_ref=target.at[me],
            send_sem=send_sem,
            recv_sem=recv_sem,
            device_id=(peer // cols, lax.rem(peer, cols)),
            device_id_type=pl.DeviceIdType.MESH,
        ).start()
        return carry

    lax.fori_loop(1, devices, send, 0)
    whole = target.at[pl.ds(0, devices - 1)]
    pltpu.make_async_copy(whole, whole, send_sem).wait()
    pltpu.make_async_copy(whole, whole, recv_sem).wait()


def swap_kernel(devices, put_ref, out_ref, held, send_sem, recv_sem):
    me = place()
    greet(devices)
    send_all(devices, lambda peer: put_ref.at[peer], held, send_sem, recv_sem)
    held[me] = put_ref[me]
    out_ref[...] = held[...]


def total_kernel(devices, put_ref, out_ref, held, mine, spread, sems):
    me = place()
    greet(devices)
    send_all(devices, lambda peer: put_ref.at[peer], held, sems.at[0], sems.at[1])
    held[me] = put_ref[me]
    mine[...] = jnp.sum(held[...], axis=0)
    send_all(devices, lambda peer: mine, spread, sems.at[2], sems.at[3])
    spread[me] = mine[...]
    out_ref[...] = spread[...]


def swap(values, ident):
    devices = values.shape[0]
    return pl.pallas_call(
        functools.partial(swap_kernel, devices),
        out_shape=jax.ShapeDtypeStruct(values.shape, jnp.float32),
        in_specs=[pl.BlockSpec(memory_space=pltpu.VMEM)],
        out_specs=pl.BlockSpec(memory_space=pltpu.VMEM),
        scratch_shapes=[pltpu.VMEM(values.shape, jnp.float32), pltpu.SemaphoreType.DMA, pltpu.SemaphoreType.DMA],
        compiler_params=pltpu.CompilerParams(collective_id=ident, has_side_effects=True),
    )(values)


def total(values, ident):
    devices = values.shape[0]
    return pl.pallas_call(
        functools.partial(total_kernel, devices),
        out_shape=jax.ShapeDtypeStruct(values.shape, jnp.float32),
        in_specs=[pl.BlockSpec(memory_space=pltpu.VMEM)],
        out_specs=pl.BlockSpec(memory_space=pltpu.VMEM),
        scratch_shapes=[
            pltpu.VMEM(values.shape, jnp.float32),
            pltpu.VMEM(values.shape[1:], jnp.float32),
            pltpu.VMEM(values.shape, jnp.float32),
            pltpu.SemaphoreType.DMA((4,)),
        ],
        compiler_params=pltpu.CompilerParams(collective_id=ident, has_side_effects=True),
    )(values)


def split(x):
    high = x.astype(jnp.bfloat16)
    return high, (x - high.astype(jnp.float32)).astype(jnp.bfloat16)


def narrow(a, b):
    return lax.dot_general(a, b, (((1,), (0,)), ((), ())), preferred_element_type=jnp.float32)


def left_split(x, high, low):
    rows = x.shape[0]
    top, rest = split(x)
    both = narrow(jnp.concatenate([top, rest], axis=0), high)
    return both[:rows] + both[rows:] + narrow(top, low)


def iota(shape, dim):
    return lax.broadcasted_iota(jnp.int32, shape, dim)


def ones_where(mask):
    return jnp.where(mask, 1.0, 0.0).astype(jnp.float32)


def store_lanes(matrix, copies, high_ref, low_ref):
    shape = (matrix.shape[1], matrix.shape[1] * copies)
    wide = dot(matrix, ones_where(iota(shape, 1) // copies == iota(shape, 0)), ((1,), (0,)))
    shape = (copies, shape[1])
    keep = iota(shape, 1) % copies == iota(shape, 0)
    for k in range(matrix.shape[0]):
        high, low = split(jnp.where(keep, jnp.broadcast_to(wide[k:k + 1, :], shape), 0.0))
        high_ref[k * copies:(k + 1) * copies, :] = high
        low_ref[k * copies:(k + 1) * copies, :] = low


def eliminate(left, right, first, last):
    size = left.shape[0]
    index = iota((size, 1), 0)
    for k in range(first, last):
        scale = lax.rsqrt(left[k:k + 1, k:k + 1])
        column = left[:, k:k + 1] * scale
        pivot_left = left[k:k + 1, :] * scale
        pivot_right = right[k:k + 1, :] * scale
        factor = jnp.where(index > k, column, 0.0)
        left = left - factor * pivot_left
        right = jnp.where(index == k, pivot_right, right - factor * pivot_right)
    return left, right


def copy_to(source, target, row, col, send_sem, recv_sem):
    pltpu.make_async_remote_copy(
        src_ref=source,
        dst_ref=target,
        send_sem=send_sem,
        recv_sem=recv_sem,
        device_id=(row, col),
        device_id_type=pl.DeviceIdType.MESH,
    ).start()


def wait_for(ref, sem):
    pltpu.make_async_copy(ref, ref, sem).wait()


def hooi_kernel(tensor_hbm, two_hbm, three_hbm, four_hbm, init_hbm, core_ref, basis_ref,
                slabs, two_ref, three_ref, four_ref, init_ref,
                high_ref, low_ref, mix_high, mix_low, hat_high, hat_low, turn_high, turn_low,
                lane_high, lane_low, twos, threes, puts, gots,
                parts, paired, sums, shares, mine, spread,
                load_sem, factor_sem, send_sem, recv_sem, image_sem, share_sem):
    rows, cols = lax.axis_size("row"), lax.axis_size("col")
    row, col = lax.axis_index("row"), lax.axis_index("col")
    devices = rows * cols
    members = devices // 2
    half = lax.rem(row, 2)
    seat = (row // 2) * cols + col
    me = row * cols + col
    partner = row + 1 - 2 * half
    rank_one, first_len = init_ref.shape
    half_len = first_len // 2
    local_two, local_three = two_ref.shape[0], three_ref.shape[0]
    rank_four, fourth_len = four_ref.shape
    width = local_three * fourth_len
    lanes = local_two * rank_four
    features = local_three * lanes
    copies = rank_one // devices
    spans = half_len // LANES

    slab_loads = [pltpu.make_async_copy(tensor_hbm.at[:, b, :], slabs.at[b], load_sem.at[b]) for b in range(local_two)]
    small = [(four_hbm, four_ref), (init_hbm, init_ref), (two_hbm, two_ref), (three_hbm, three_ref)]
    small_loads = [pltpu.make_async_copy(source, target, load_sem.at[local_two + k]) for k, (source, target) in enumerate(small)]
    small_loads[0].start()
    small_loads[1].start()
    for load in slab_loads:
        load.start()
    small_loads[2].start()
    small_loads[3].start()

    def target(k):
        turn = k // (rows // 2)
        shift = (turn + 1) // 2
        there = lax.rem(col + cols // 2 + cols + (1 - 2 * lax.rem(turn, 2)) * shift, cols)
        return lax.rem(row // 2 + rows - 1 - lax.rem(k, rows // 2), rows // 2), there

    def at(index, count):
        return pl.ds(pl.multiple_of(index * count, count), count)

    barrier = pltpu.get_barrier_semaphore()

    def greet_at(there_row, there_col):
        pl.semaphore_signal(barrier, inc=1, device_id=(there_row, there_col), device_id_type=pl.DeviceIdType.MESH)

    def hello(k, carry):
        there_row, there_col = target(k)
        greet_at(there_row * 2, there_col)
        greet_at(there_row * 2 + 1, there_col)
        return carry

    def hello_near(k, carry):
        greet_at(lax.rem(row + k, rows), col)
        return carry

    lax.fori_loop(0, members - rows // 2, hello, 0, unroll=True)
    lax.fori_loop(1, rows, hello_near, 0, unroll=True)

    small_loads[0].wait()
    lane = iota((fourth_len, features), 1)
    shape = (rank_four, features)
    four = dot(four_ref[...], ones_where(iota(shape, 1) % rank_four == iota(shape, 0)), ((0,), (0,)))
    four_high = four.astype(jnp.bfloat16).astype(jnp.float32)
    four_low = four - four_high
    for b in range(local_two):
        for c in range(local_three):
            keep = lane // rank_four == c * local_two + b
            part = slice((b * local_three + c) * fourth_len, (b * local_three + c + 1) * fourth_len)
            mix_high[part, :] = jnp.where(keep, four_high, 0.0).astype(jnp.bfloat16)
            mix_low[part, :] = jnp.where(keep, four_low, 0.0).astype(jnp.bfloat16)

    small_loads[1].wait()
    init_high, init_low = split(init_ref[...])
    init_both = jnp.concatenate([init_high, init_low], axis=0)
    cuts = [0, local_two // 2, local_two]
    count = len(cuts) - 1

    def span_of(k):
        return slice(cuts[k] * width, cuts[k + 1] * width)

    def pull_group(k):
        both = narrow(init_both, high_ref[:, span_of(k)])
        return both[:rank_one] + both[rank_one:] + narrow(init_high, low_ref[:, span_of(k)])

    pulled, vectors = [], []
    for k in range(count + 2):
        if k < count:
            for b in range(cuts[k], cuts[k + 1]):
                slab_loads[b].wait()
                high, low = split(slabs[b])
                high_ref[:, b * width:(b + 1) * width] = high
                low_ref[:, b * width:(b + 1) * width] = low
        if k >= 2:
            vectors.append(left_split(pulled[k - 2], mix_high[span_of(k - 2), :], mix_low[span_of(k - 2), :]))
        if 1 <= k <= count:
            pulled.append(pull_group(k - 1))
    vectors = sum(vectors[1:], vectors[0])

    def flat(ref):
        return ref.reshape(devices * local_three, lanes)

    def deal(vectors, put):
        for c in range(local_three):
            put[pl.ds(c, devices, stride=local_three), :] = vectors[:, c * lanes:(c + 1) * lanes]

    def send(stage, k):
        put, got = puts.at[stage, k], gots.at[stage, k]

        def one(there_row, there_col):
            copy_to(put.at[there_row * cols + there_col], got.at[me], there_row, there_col, send_sem.at[stage, k], recv_sem.at[stage, k])

        for h in range(2):
            def some(i, carry):
                there_row, there_col = target(i)
                one(there_row * 2 + h, there_col)
                return carry

            lax.fori_loop(0, members - 1, some, 0, unroll=True)
        one(partner, col)
        got[me] = put[me]

    def arrive(stage, k):
        wait_for(gots.at[stage, k, pl.ds(0, devices - 1)], recv_sem.at[stage, k])

    def contract(stage, k, matrix):
        got, put = flat(gots.at[stage, k]), flat(puts.at[stage + 1, k])
        size = cols * local_three
        top, rest = split(jnp.concatenate([got[i * size:(i + 1) * size, :] for i in range(rows)], axis=1))
        result = left_split(narrow(matrix, jnp.concatenate([top, top, rest], axis=0)), lane_high[...], lane_low[...])
        for i in range(rows):
            put[i * size:(i + 1) * size, :] = result[:, i * lanes:(i + 1) * lanes]

    def triple(matrix, axis):
        high, low = split(matrix)
        return jnp.concatenate([high, low, high], axis=axis)

    def collect(stage, k):
        got = flat(gots.at[stage, k])
        return jnp.concatenate([got[pl.ds(c, devices, stride=local_three), :] for c in range(local_three)], axis=1)

    for k in range(copies):
        deal(vectors[k * devices:(k + 1) * devices], flat(puts.at[0, k]))
    small_loads[2].wait()
    small_loads[3].wait()
    pl.semaphore_wait(barrier, devices - 1)

    def send_two(k, carry):
        copy_to(two_ref, twos.at[row], lax.rem(row + k, rows), col, factor_sem.at[0], factor_sem.at[1])
        return carry

    def send_three(k, carry):
        copy_to(three_ref, threes.at[col], row, lax.rem(col + k, cols), factor_sem.at[2], factor_sem.at[3])
        return carry

    lax.fori_loop(1, rows, send_two, 0, unroll=True)
    lax.fori_loop(1, cols, send_three, 0, unroll=True)
    for k in range(copies):
        send(0, k)
    twos[row] = two_ref[...]
    threes[col] = three_ref[...]

    def hat_piece(k, count):
        part = slice(k * first_len // count, (k + 1) * first_len // count)
        hat = narrow(high_ref[part, :], mix_high[...]) + narrow(high_ref[part, :], mix_low[...]) + narrow(low_ref[part, :], mix_high[...])
        hat_high[part, :], hat_low[part, :] = split(hat)
        turn_high[:, part], turn_low[:, part] = split(hat.T)

    hat_piece(0, 4)
    wait_for(twos.at[pl.ds(0, rows - 1)], factor_sem.at[1])
    wait_for(threes.at[pl.ds(0, cols - 1)], factor_sem.at[3])
    whole_two = jnp.concatenate([twos[k] for k in range(rows)], axis=0)
    whole_three = jnp.concatenate([threes[k] for k in range(cols)], axis=0)
    store_lanes(dot(whole_two, whole_two, ((1,), (1,))), rank_four, lane_high, lane_low)
    left = triple(dot(whole_three, whole_three, ((1,), (1,))), 1)

    for k in range(copies):
        arrive(0, k)
        contract(0, k, left)
        send(1, k)
    hat_piece(1, 4)
    hat_piece(2, 4)
    hat_piece(3, 4)

    def tiles():
        for i in range(members):
            r, w = i // spans, i % spans
            yield i, slice(r * 8, (r + 1) * 8), slice(w * LANES, (w + 1) * LANES)

    owned = []
    for k in range(copies):
        arrive(1, k)
        back = collect(1, k)
        span = at(1 - half, half_len)
        image = left_split(back, turn_high[:, span], turn_low[:, span])
        for i, r, w in tiles():
            parts[k, i] = image[r, w]
        copy_to(parts.at[k], paired.at[k], partner, col, share_sem.at[4, k], share_sem.at[5, k])
        span = at(half, half_len)
        owned.append(left_split(back, turn_high[:, span], turn_low[:, span]))

    for k in range(copies):
        wait_for(paired.at[k], share_sem.at[5, k])
        for i, r, w in tiles():
            sums[k, i] = owned[k][r, w] + paired[k, i]

        def scatter(i, carry):
            there_row, there_col = target(i)
            copy_to(sums.at[k, there_row * cols + there_col], shares.at[k, seat], there_row * 2 + 1 - half, there_col, share_sem.at[0, k], share_sem.at[1, k])
            return carry

        lax.fori_loop(0, members, scatter, 0, unroll=True)
    for k in range(copies):
        wait_for(shares.at[k], share_sem.at[1, k])
        mine[k] = jnp.sum(shares[k], axis=0)

        def gather(i, carry):
            there_row, there_col = target(i)
            copy_to(mine.at[k], spread.at[1 - half, k, seat], there_row * 2 + 1 - half, there_col, share_sem.at[2, k], share_sem.at[3, k])
            return carry

        lax.fori_loop(0, members, gather, 0, unroll=True)
    def image_half(which, k):
        return jnp.concatenate([
            jnp.concatenate([spread[which, k, r * spans + w] for w in range(spans)], axis=1)
            for r in range(members // spans)], axis=0)

    def pull_half(which, k):
        span = at(which, half_len)
        return left_split(image_half(which, k), hat_high[span, :], hat_low[span, :])

    def pass_on(k):
        wait_for(spread.at[half, k], share_sem.at[3, k])
        copy_to(spread.at[half, k], spread.at[half, k], partner, col, image_sem.at[0, k], image_sem.at[1, k])

    pass_on(0)
    for k in range(copies):
        vectors = pull_half(half, k)
        if k + 1 < copies:
            pass_on(k + 1)
        wait_for(spread.at[1 - half, k], image_sem.at[1, k])
        deal(vectors + pull_half(1 - half, k), flat(puts.at[2, k]))
        send(2, k)

    image = jnp.concatenate([jnp.concatenate([image_half(0, k), image_half(1, k)], axis=1) for k in range(copies)], axis=0)
    lower = dot(image, image, ((1,), (1,)))
    shape = lower.shape
    lower, inverse = eliminate(lower, ones_where(iota(shape, 0) == iota(shape, 1)), 0, rank_one * 5 // 8)
    store_lanes(whole_two, rank_four, lane_high, lane_low)
    left = triple(whole_three.T, 1)
    for k in range(copies):
        arrive(2, k)
        contract(2, k, left)
        send(3, k)
    lower, inverse = eliminate(lower, inverse, rank_one * 5 // 8, rank_one)
    basis_ref[...] = dot(inverse, image, ((1,), (0,)))
    inverse_high, inverse_low = split(inverse.T)
    weights = jnp.concatenate([inverse_high, inverse_high, inverse_low], axis=0)
    for k in range(copies):
        arrive(3, k)
    vectors = jnp.concatenate([collect(3, k) for k in range(copies)], axis=0)
    core = lax.dot_general(triple(vectors, 0), weights, (((0,), (0,)), ((), ())), preferred_element_type=jnp.float32)
    for c in range(local_three):
        for b in range(local_two):
            core_ref[b, c] = core[(c * local_two + b) * rank_four:(c * local_two + b + 1) * rank_four, :]

    for k in range(copies):
        for stage in range(4):
            wait_for(gots.at[stage, k, pl.ds(0, devices - 1)], send_sem.at[stage, k])
        wait_for(paired.at[k], share_sem.at[4, k])
        wait_for(shares.at[k], share_sem.at[0, k])
        wait_for(shares.at[k], share_sem.at[2, k])
        wait_for(paired.at[k], image_sem.at[0, k])
    wait_for(twos.at[pl.ds(0, rows - 1)], factor_sem.at[0])
    wait_for(threes.at[pl.ds(0, cols - 1)], factor_sem.at[2])


def write_kernel(core_ref, basis_ref, core_hbm, basis_hbm, sem):
    first = pltpu.make_async_copy(core_ref, core_hbm, sem.at[0])
    second = pltpu.make_async_copy(basis_ref, basis_hbm, sem.at[1])
    first.start()
    second.start()
    first.wait()
    second.wait()


def fits(tensor, factor_two, factor_three, factor_four, factor_init):
    rows, cols = lax.axis_size("row"), lax.axis_size("col")
    devices = rows * cols
    first_len, local_two, width = tensor.shape
    fourth_len, rank_four = factor_four.shape
    rank_one = factor_init.shape[1]
    local_three = width // fourth_len
    same = factor_two.shape[1] == local_two * rows and factor_three.shape[1] == local_three * cols
    even = rows % 2 == 0 and cols % 2 == 0 and rank_one % devices == 0
    flat = local_two * rank_four == LANES and width == LANES and (local_three == 4 or local_three % 8 == 0)
    tiles = (devices // 8) * (first_len // (2 * LANES))
    return same and even and flat and first_len % (4 * LANES) == 0 and devices % 8 == 0 and tiles == devices // 2


def fused(tensor, factor_two, factor_three, factor_four, factor_init):
    rows, cols = lax.axis_size("row"), lax.axis_size("col")
    devices = rows * cols
    members = devices // 2
    first_len, local_two, width = tensor.shape
    fourth_len, rank_four = factor_four.shape
    rank_one = factor_init.shape[1]
    local_three = width // fourth_len
    lanes = local_two * rank_four
    features = local_three * lanes
    total_width = local_two * width
    copies = rank_one // devices
    wide = rows * lanes

    def f32(*shape):
        return pltpu.VMEM(shape, jnp.float32)

    def bf16(*shape):
        return pltpu.VMEM(shape, jnp.bfloat16)

    vmem, hbm = pl.BlockSpec(memory_space=pltpu.VMEM), pl.BlockSpec(memory_space=pltpu.HBM)
    shapes = (
        jax.ShapeDtypeStruct((local_two, local_three, rank_four, rank_one), jnp.float32),
        jax.ShapeDtypeStruct((rank_one, first_len), jnp.float32),
    )
    operands = [pltpu.with_memory_space_constraint(x, pltpu.HBM) for x in (tensor, factor_two, factor_three, factor_four.T, factor_init.T)]
    core, basis = pl.pallas_call(
        hooi_kernel,
        out_shape=tuple(pltpu.VMEM(x.shape, x.dtype) for x in shapes),
        in_specs=[hbm] * 5,
        out_specs=(vmem, vmem),
        scratch_shapes=[
            f32(local_two, first_len, width), f32(*factor_two.shape), f32(*factor_three.shape), f32(rank_four, fourth_len), f32(rank_one, first_len),
            bf16(first_len, total_width), bf16(first_len, total_width), bf16(total_width, features), bf16(total_width, features),
            bf16(first_len, features), bf16(first_len, features), bf16(features, first_len), bf16(features, first_len),
            bf16(wide, wide), bf16(wide, wide), f32(rows, *factor_two.shape), f32(cols, *factor_three.shape),
            f32(4, copies, devices, local_three, lanes), f32(4, copies, devices, local_three, lanes),
            f32(copies, members, 8, LANES), f32(copies, members, 8, LANES), f32(copies, members, 8, LANES), f32(copies, members, 8, LANES),
            f32(copies, 8, LANES), f32(2, copies, members, 8, LANES),
            pltpu.SemaphoreType.DMA((local_two + 4,)),
            pltpu.SemaphoreType.DMA((4,)),
            pltpu.SemaphoreType.DMA((4, copies)),
            pltpu.SemaphoreType.DMA((4, copies)),
            pltpu.SemaphoreType.DMA((2, copies)),
            pltpu.SemaphoreType.DMA((6, copies)),
        ],
        compiler_params=pltpu.CompilerParams(collective_id=0, has_side_effects=True, vmem_limit_bytes=48 << 20),
    )(*operands)
    core, basis = pl.pallas_call(
        write_kernel,
        out_shape=shapes,
        in_specs=[vmem, vmem],
        out_specs=(hbm, hbm),
        scratch_shapes=[pltpu.SemaphoreType.DMA((2,))],
        compiler_params=pltpu.CompilerParams(vmem_limit_bytes=4 << 20),
    )(core, basis)
    return basis.T, core.transpose(3, 0, 1, 2)


def shards(tensor, factor_two, factor_three, factor_four, factor_init):
    if fits(tensor, factor_two, factor_three, factor_four, factor_init):
        return fused(tensor, factor_two, factor_three, factor_four, factor_init)
    axes = ("row", "col")
    first_len, local_two, width = tensor.shape
    fourth_len, rank_four = factor_four.shape
    local_three = width // fourth_len
    rank_one = factor_init.shape[1]
    rows, cols = lax.axis_size("row"), lax.axis_size("col")
    devices = rows * cols
    local_pairs = local_two * local_three
    features = rank_four * rank_one
    part = features // devices
    data = tensor.reshape(first_len, local_pairs, fourth_len)
    rank_two, rank_three = factor_two.shape[1], factor_three.shape[1]

    def pull(vectors):
        mixed = jnp.einsum("apd,ar->prd", data, vectors, precision=lax.Precision.HIGH)
        return jnp.einsum("prd,de->per", mixed, factor_four, precision=HIGHEST).reshape(local_pairs, features)

    def share(values, ident):
        length = values.shape[1]
        padded = -(-length // LANES) * LANES
        values = jnp.pad(values, ((0, 0), (0, padded - length))).reshape(devices, padded // LANES, LANES)
        return swap(values, ident).reshape(devices, padded)[:, :length]

    def spread(block, ident, extra=None):
        put = block.reshape(local_pairs, devices, part).transpose(1, 0, 2).reshape(devices, local_pairs * part)
        if extra is not None:
            put = jnp.concatenate([put, jnp.broadcast_to(extra[None], (devices, extra.shape[0]))], axis=1)
        got = share(put, ident)
        rest = got[:, local_pairs * part:]
        got = got[:, :local_pairs * part]
        got = got.reshape(rows, cols, local_two, local_three, part)
        return got.transpose(0, 2, 1, 3, 4).reshape(rows * local_two, cols * local_three, part), rest

    def gather(block, ident):
        two, three, _ = block.shape
        put = block.reshape(rows, two // rows, cols, three // cols, part).transpose(0, 2, 1, 3, 4)
        got = share(put.reshape(devices, -1), ident).reshape(devices, (two // rows) * (three // cols), part)
        return got.transpose(1, 0, 2).reshape(got.shape[1], features)

    extra = jnp.concatenate([factor_two.reshape(-1), factor_three.reshape(-1)])
    block, rest = spread(pull(factor_init), 1, extra)
    rest = rest.reshape(rows, cols, -1)
    whole_two = rest[:, 0, :factor_two.size].reshape(-1, rank_two)
    whole_three = rest[0, :, factor_two.size:].reshape(-1, rank_three)
    block = jnp.einsum("bcq,bg->gcq", block, whole_two, precision=HIGHEST)
    block = jnp.einsum("gcq,cf->gfq", block, whole_three, precision=HIGHEST)
    block = jnp.einsum("gfq,cf->gcq", block, whole_three, precision=HIGHEST)
    block = jnp.einsum("gcq,bg->bcq", block, whole_two, precision=HIGHEST)
    block = gather(block, 2).reshape(local_pairs, rank_four, rank_one)
    block = jnp.einsum("per,de->pdr", block, factor_four, precision=HIGHEST)
    image = jnp.dot(tensor.reshape(first_len, -1), block.reshape(-1, rank_one), precision=lax.Precision.HIGH)
    half = first_len // 2
    image = jnp.concatenate([image[:half], image[half:]], axis=1).reshape(devices, half // devices, 2 * rank_one)
    image = total(image, 0).reshape(half, 2 * rank_one)
    image = jnp.concatenate([image[:, :rank_one], image[:, rank_one:]], axis=0)
    basis, inverse = finish(image)
    block, _ = spread(pull(image), 3)
    block = jnp.einsum("bcq,bg->gcq", block, whole_two, precision=HIGHEST)
    block = jnp.einsum("gcq,cf->gfq", block, whole_three, precision=HIGHEST)
    block = gather(block, 4).reshape(-1, rank_four, rank_one)
    core = jnp.einsum("per,sr->spe", block, inverse, precision=HIGHEST)
    return (basis, core.reshape(rank_one, rank_two // rows, rank_three // cols, rank_four))


def solution(mesh):
    in_specs = (P(None, "row", "col"), P("row", None), P("col", None), P(), P())
    out_specs = (P(), P(None, "row", "col", None))
    return jax.shard_map(shards, mesh=mesh, in_specs=in_specs, out_specs=out_specs, check_vma=False)
```

```python
import functools

import jax
import jax.numpy as jnp
from jax import lax
from jax.experimental import pallas as pl
from jax.experimental.pallas import tpu as pltpu
from jax.sharding import PartitionSpec as P

HIGHEST = lax.Precision.HIGHEST
LANES = 128


def dot(a, b, dims):
    return lax.dot_general(a, b, (dims, ((), ())), precision=HIGHEST, preferred_element_type=jnp.float32)


def inverse_factor(square):
    size = square.shape[0]
    rows = lax.broadcasted_iota(jnp.int32, (size, size), 0)
    cols = lax.broadcasted_iota(jnp.int32, (size, size), 1)
    index = lax.broadcasted_iota(jnp.int32, (size, 1), 0)
    left = square
    right = jnp.where(rows == cols, 1.0, 0.0).astype(jnp.float32)
    for k in range(size):
        scale = lax.rsqrt(left[k:k + 1, k:k + 1])
        column = left[:, k:k + 1] * scale
        pivot_left = left[k:k + 1, :] * scale
        pivot_right = right[k:k + 1, :] * scale
        factor = jnp.where(index > k, column, 0.0)
        left = left - factor * pivot_left
        right = jnp.where(index == k, pivot_right, right - factor * pivot_right)
    return right


def finish_kernel(image_ref, basis_ref, inverse_ref):
    image = image_ref[...]
    inverse = inverse_factor(dot(image, image, ((0,), (0,))))
    inverse_ref[...] = inverse
    basis_ref[...] = dot(image, inverse, ((1,), (1,)))


def finish(image):
    rank = image.shape[1]
    return pl.pallas_call(
        finish_kernel,
        out_shape=(
            jax.ShapeDtypeStruct(image.shape, jnp.float32),
            jax.ShapeDtypeStruct((rank, rank), jnp.float32),
        ),
    )(image)


def place():
    return lax.axis_index("row") * lax.axis_size("col") + lax.axis_index("col")


def greet(devices):
    cols = lax.axis_size("col")
    me = place()
    barrier = pltpu.get_barrier_semaphore()

    def hello(k, carry):
        peer = lax.rem(me + k, devices)
        pl.semaphore_signal(barrier, inc=1, device_id=(peer // cols, lax.rem(peer, cols)), device_id_type=pl.DeviceIdType.MESH)
        return carry

    lax.fori_loop(1, devices, hello, 0)
    pl.semaphore_wait(barrier, devices - 1)


def send_all(devices, source, target, send_sem, recv_sem):
    cols = lax.axis_size("col")
    me = place()

    def send(k, carry):
        peer = lax.rem(me + k, devices)
        pltpu.make_async_remote_copy(
            src_ref=source(peer),
            dst_ref=target.at[me],
            send_sem=send_sem,
            recv_sem=recv_sem,
            device_id=(peer // cols, lax.rem(peer, cols)),
            device_id_type=pl.DeviceIdType.MESH,
        ).start()
        return carry

    lax.fori_loop(1, devices, send, 0)
    whole = target.at[pl.ds(0, devices - 1)]
    pltpu.make_async_copy(whole, whole, send_sem).wait()
    pltpu.make_async_copy(whole, whole, recv_sem).wait()


def swap_kernel(devices, put_ref, out_ref, held, send_sem, recv_sem):
    me = place()
    greet(devices)
    send_all(devices, lambda peer: put_ref.at[peer], held, send_sem, recv_sem)
    held[me] = put_ref[me]
    out_ref[...] = held[...]


def total_kernel(devices, put_ref, out_ref, held, mine, spread, sems):
    me = place()
    greet(devices)
    send_all(devices, lambda peer: put_ref.at[peer], held, sems.at[0], sems.at[1])
    held[me] = put_ref[me]
    mine[...] = jnp.sum(held[...], axis=0)
    send_all(devices, lambda peer: mine, spread, sems.at[2], sems.at[3])
    spread[me] = mine[...]
    out_ref[...] = spread[...]


def swap(values, ident):
    devices = values.shape[0]
    return pl.pallas_call(
        functools.partial(swap_kernel, devices),
        out_shape=jax.ShapeDtypeStruct(values.shape, jnp.float32),
        in_specs=[pl.BlockSpec(memory_space=pltpu.VMEM)],
        out_specs=pl.BlockSpec(memory_space=pltpu.VMEM),
        scratch_shapes=[pltpu.VMEM(values.shape, jnp.float32), pltpu.SemaphoreType.DMA, pltpu.SemaphoreType.DMA],
        compiler_params=pltpu.CompilerParams(collective_id=ident, has_side_effects=True),
    )(values)


def total(values, ident):
    devices = values.shape[0]
    return pl.pallas_call(
        functools.partial(total_kernel, devices),
        out_shape=jax.ShapeDtypeStruct(values.shape, jnp.float32),
        in_specs=[pl.BlockSpec(memory_space=pltpu.VMEM)],
        out_specs=pl.BlockSpec(memory_space=pltpu.VMEM),
        scratch_shapes=[
            pltpu.VMEM(values.shape, jnp.float32),
            pltpu.VMEM(values.shape[1:], jnp.float32),
            pltpu.VMEM(values.shape, jnp.float32),
            pltpu.SemaphoreType.DMA((4,)),
        ],
        compiler_params=pltpu.CompilerParams(collective_id=ident, has_side_effects=True),
    )(values)


def split(x):
    high = x.astype(jnp.bfloat16)
    return high, (x - high.astype(jnp.float32)).astype(jnp.bfloat16)


def narrow(a, b):
    return lax.dot_general(a, b, (((1,), (0,)), ((), ())), preferred_element_type=jnp.float32)


def left_split(x, high, low):
    rows = x.shape[0]
    top, rest = split(x)
    both = narrow(jnp.concatenate([top, rest], axis=0), high)
    return both[:rows] + both[rows:] + narrow(top, low)


def iota(shape, dim):
    return lax.broadcasted_iota(jnp.int32, shape, dim)


def ones_where(mask):
    return jnp.where(mask, 1.0, 0.0).astype(jnp.float32)


def store_lanes(matrix, copies, high_ref, low_ref):
    shape = (matrix.shape[1], matrix.shape[1] * copies)
    wide = dot(matrix, ones_where(iota(shape, 1) // copies == iota(shape, 0)), ((1,), (0,)))
    shape = (copies, shape[1])
    keep = iota(shape, 1) % copies == iota(shape, 0)
    for k in range(matrix.shape[0]):
        high, low = split(jnp.where(keep, jnp.broadcast_to(wide[k:k + 1, :], shape), 0.0))
        high_ref[k * copies:(k + 1) * copies, :] = high
        low_ref[k * copies:(k + 1) * copies, :] = low


def eliminate(left, right, first, last):
    size = left.shape[0]
    index = iota((size, 1), 0)
    for k in range(first, last):
        scale = lax.rsqrt(left[k:k + 1, k:k + 1])
        column = left[:, k:k + 1] * scale
        pivot_left = left[k:k + 1, :] * scale
        pivot_right = right[k:k + 1, :] * scale
        factor = jnp.where(index > k, column, 0.0)
        left = left - factor * pivot_left
        right = jnp.where(index == k, pivot_right, right - factor * pivot_right)
    return left, right


def copy_to(source, target, row, col, send_sem, recv_sem):
    pltpu.make_async_remote_copy(
        src_ref=source,
        dst_ref=target,
        send_sem=send_sem,
        recv_sem=recv_sem,
        device_id=(row, col),
        device_id_type=pl.DeviceIdType.MESH,
    ).start()


def wait_for(ref, sem):
    pltpu.make_async_copy(ref, ref, sem).wait()


def hooi_kernel(tensor_hbm, two_hbm, three_hbm, four_hbm, init_hbm, core_ref, basis_ref,
                slabs, two_ref, three_ref, four_ref, init_ref,
                high_ref, low_ref, mix_high, mix_low, hat_high, hat_low, turn_high, turn_low,
                lane_high, lane_low, twos, threes, puts, gots,
                parts, paired, sums, shares, mine, spread,
                load_sem, factor_sem, send_sem, recv_sem, image_sem, share_sem):
    rows, cols = lax.axis_size("row"), lax.axis_size("col")
    row, col = lax.axis_index("row"), lax.axis_index("col")
    devices = rows * cols
    members = devices // 2
    half = lax.rem(row, 2)
    seat = (row // 2) * cols + col
    me = row * cols + col
    partner = row + 1 - 2 * half
    rank_one, first_len = init_ref.shape
    half_len = first_len // 2
    local_two, local_three = two_ref.shape[0], three_ref.shape[0]
    rank_four, fourth_len = four_ref.shape
    width = local_three * fourth_len
    lanes = local_two * rank_four
    features = local_three * lanes
    copies = rank_one // devices
    spans = half_len // LANES

    slab_loads = [pltpu.make_async_copy(tensor_hbm.at[:, b, :], slabs.at[b], load_sem.at[b]) for b in range(local_two)]
    small = [(four_hbm, four_ref), (init_hbm, init_ref), (two_hbm, two_ref), (three_hbm, three_ref)]
    small_loads = [pltpu.make_async_copy(source, target, load_sem.at[local_two + k]) for k, (source, target) in enumerate(small)]
    small_loads[0].start()
    small_loads[1].start()
    for load in slab_loads:
        load.start()
    small_loads[2].start()
    small_loads[3].start()

    def target(k):
        turn = k // (rows // 2)
        shift = (turn + 1) // 2
        there = lax.rem(col + cols // 2 + cols + (1 - 2 * lax.rem(turn, 2)) * shift, cols)
        return lax.rem(row // 2 + rows - 1 - lax.rem(k, rows // 2), rows // 2), there

    def at(index, count):
        return pl.ds(pl.multiple_of(index * count, count), count)

    barrier = pltpu.get_barrier_semaphore()

    def greet_at(there_row, there_col):
        pl.semaphore_signal(barrier, inc=1, device_id=(there_row, there_col), device_id_type=pl.DeviceIdType.MESH)

    def hello(k, carry):
        there_row, there_col = target(k)
        greet_at(there_row * 2, there_col)
        greet_at(there_row * 2 + 1, there_col)
        return carry

    def hello_near(k, carry):
        greet_at(lax.rem(row + k, rows), col)
        return carry

    lax.fori_loop(0, members - rows // 2, hello, 0, unroll=True)
    lax.fori_loop(1, rows, hello_near, 0, unroll=True)

    small_loads[0].wait()
    lane = iota((fourth_len, features), 1)
    shape = (rank_four, features)
    four = dot(four_ref[...], ones_where(iota(shape, 1) % rank_four == iota(shape, 0)), ((0,), (0,)))
    four_high = four.astype(jnp.bfloat16).astype(jnp.float32)
    four_low = four - four_high
    for b in range(local_two):
        for c in range(local_three):
            keep = lane // rank_four == c * local_two + b
            part = slice((b * local_three + c) * fourth_len, (b * local_three + c + 1) * fourth_len)
            mix_high[part, :] = jnp.where(keep, four_high, 0.0).astype(jnp.bfloat16)
            mix_low[part, :] = jnp.where(keep, four_low, 0.0).astype(jnp.bfloat16)

    small_loads[1].wait()
    init_high, init_low = split(init_ref[...])
    init_both = jnp.concatenate([init_high, init_low], axis=0)
    cuts = [0, local_two // 2, local_two]
    count = len(cuts) - 1

    def span_of(k):
        return slice(cuts[k] * width, cuts[k + 1] * width)

    def pull_group(k):
        both = narrow(init_both, high_ref[:, span_of(k)])
        return both[:rank_one] + both[rank_one:] + narrow(init_high, low_ref[:, span_of(k)])

    pulled, vectors = [], []
    for k in range(count + 2):
        if k < count:
            for b in range(cuts[k], cuts[k + 1]):
                slab_loads[b].wait()
                high, low = split(slabs[b])
                high_ref[:, b * width:(b + 1) * width] = high
                low_ref[:, b * width:(b + 1) * width] = low
        if k >= 2:
            vectors.append(left_split(pulled[k - 2], mix_high[span_of(k - 2), :], mix_low[span_of(k - 2), :]))
        if 1 <= k <= count:
            pulled.append(pull_group(k - 1))
    vectors = sum(vectors[1:], vectors[0])

    def fenced(body):
        def trip(_, carry):
            body()
            return carry

        lax.fori_loop(0, 1 + me // devices, trip, 0)

    def flat(ref):
        return ref.reshape(devices * local_three, lanes)

    def deal(vectors, put):
        for c in range(local_three):
            put[pl.ds(c, devices, stride=local_three), :] = vectors[:, c * lanes:(c + 1) * lanes]

    def send(stage, k):
        put, got = puts.at[stage, k], gots.at[stage, k]

        def one(there_row, there_col):
            copy_to(put.at[there_row * cols + there_col], got.at[me], there_row, there_col, send_sem.at[stage, k], recv_sem.at[stage, k])

        @fenced
        def _():
            for h in range(2):
                for i in range(members - 1):
                    there_row, there_col = target(i)
                    one(there_row * 2 + h, there_col)
            one(partner, col)

        got[me] = put[me]

    def arrive(stage, k):
        wait_for(gots.at[stage, k, pl.ds(0, devices - 1)], recv_sem.at[stage, k])

    def contract(stage, k, matrix):
        got, put = flat(gots.at[stage, k]), flat(puts.at[stage + 1, k])
        size = cols * local_three
        top, rest = split(jnp.concatenate([got[i * size:(i + 1) * size, :] for i in range(rows)], axis=1))
        result = left_split(narrow(matrix, jnp.concatenate([top, top, rest], axis=0)), lane_high[...], lane_low[...])
        for i in range(rows):
            put[i * size:(i + 1) * size, :] = result[:, i * lanes:(i + 1) * lanes]

    def triple(matrix, axis):
        high, low = split(matrix)
        return jnp.concatenate([high, low, high], axis=axis)

    def collect(stage, k):
        got = flat(gots.at[stage, k])
        return jnp.concatenate([got[pl.ds(c, devices, stride=local_three), :] for c in range(local_three)], axis=1)

    for k in range(copies):
        deal(vectors[k * devices:(k + 1) * devices], flat(puts.at[0, k]))
    small_loads[2].wait()
    small_loads[3].wait()
    pl.semaphore_wait(barrier, devices - 1)

    def send_two(k, carry):
        copy_to(two_ref, twos.at[row], lax.rem(row + k, rows), col, factor_sem.at[0], factor_sem.at[1])
        return carry

    def send_three(k, carry):
        copy_to(three_ref, threes.at[col], row, lax.rem(col + k, cols), factor_sem.at[2], factor_sem.at[3])
        return carry

    lax.fori_loop(1, rows, send_two, 0, unroll=True)
    lax.fori_loop(1, cols, send_three, 0, unroll=True)
    for k in range(copies):
        send(0, k)
    twos[row] = two_ref[...]
    threes[col] = three_ref[...]

    def hat_piece(k, count):
        part = slice(k * first_len // count, (k + 1) * first_len // count)
        hat = narrow(high_ref[part, :], mix_high[...]) + narrow(high_ref[part, :], mix_low[...]) + narrow(low_ref[part, :], mix_high[...])
        hat_high[part, :], hat_low[part, :] = split(hat)
        turn_high[:, part], turn_low[:, part] = split(hat.T)

    hat_piece(0, 4)
    wait_for(twos.at[pl.ds(0, rows - 1)], factor_sem.at[1])
    wait_for(threes.at[pl.ds(0, cols - 1)], factor_sem.at[3])
    whole_two = jnp.concatenate([twos[k] for k in range(rows)], axis=0)
    whole_three = jnp.concatenate([threes[k] for k in range(cols)], axis=0)
    store_lanes(dot(whole_two, whole_two, ((1,), (1,))), rank_four, lane_high, lane_low)
    left = triple(dot(whole_three, whole_three, ((1,), (1,))), 1)

    for k in range(copies):
        arrive(0, k)
        contract(0, k, left)
        send(1, k)
    hat_piece(1, 4)
    hat_piece(2, 4)
    hat_piece(3, 4)

    def tiles():
        for i in range(members):
            r, w = i // spans, i % spans
            yield i, slice(r * 8, (r + 1) * 8), slice(w * LANES, (w + 1) * LANES)

    def image_part(back, which):
        span = at(which, half_len)
        return left_split(back, turn_high[:, span], turn_low[:, span])

    def image_out(k):
        back = collect(1, k)
        image = image_part(back, 1 - half)
        for i, r, w in tiles():
            parts[k, i] = image[r, w]
        fenced(lambda: copy_to(parts.at[k], paired.at[k], partner, col, share_sem.at[4, k], share_sem.at[5, k]))
        return back

    def scatter(k, image):
        wait_for(paired.at[k], share_sem.at[5, k])
        for i, r, w in tiles():
            sums[k, i] = image[r, w] + paired[k, i]

        @fenced
        def _():
            for i in range(members):
                there_row, there_col = target(i)
                copy_to(sums.at[k, there_row * cols + there_col], shares.at[k, seat], there_row * 2 + 1 - half, there_col, share_sem.at[0, k], share_sem.at[1, k])

    arrive(1, 0)
    owned = image_part(image_out(0), half)
    for k in range(copies):
        if k + 1 < copies:
            arrive(1, k + 1)
            back = image_out(k + 1)
        scatter(k, owned)
        if k + 1 < copies:
            owned = image_part(back, half)

    store_lanes(whole_two, rank_four, lane_high, lane_low)
    left = triple(whole_three.T, 1)
    for k in range(copies):
        wait_for(shares.at[k], share_sem.at[1, k])
        mine[k] = jnp.sum(shares[k], axis=0)

        @fenced
        def _():
            for i in range(members):
                there_row, there_col = target(i)
                copy_to(mine.at[k], spread.at[1 - half, k, seat], there_row * 2 + 1 - half, there_col, share_sem.at[2, k], share_sem.at[3, k])

    def image_half(which, k):
        return jnp.concatenate([
            jnp.concatenate([spread[which, k, r * spans + w] for w in range(spans)], axis=1)
            for r in range(members // spans)], axis=0)

    def pull_half(which, k):
        span = at(which, half_len)
        return left_split(image_half(which, k), hat_high[span, :], hat_low[span, :])

    def pass_on(k):
        wait_for(spread.at[half, k], share_sem.at[3, k])
        fenced(lambda: copy_to(spread.at[half, k], spread.at[half, k], partner, col, image_sem.at[0, k], image_sem.at[1, k]))

    pass_on(0)
    for k in range(copies):
        vectors = pull_half(half, k)
        if k + 1 < copies:
            pass_on(k + 1)
        wait_for(spread.at[1 - half, k], image_sem.at[1, k])
        deal(vectors + pull_half(1 - half, k), flat(puts.at[2, k]))
        send(2, k)

    image = jnp.concatenate([jnp.concatenate([image_half(0, k), image_half(1, k)], axis=1) for k in range(copies)], axis=0)
    lower = dot(image, image, ((1,), (1,)))
    shape = lower.shape
    lower, inverse = eliminate(lower, ones_where(iota(shape, 0) == iota(shape, 1)), 0, rank_one * 3 // 8)
    for k in range(copies):
        arrive(2, k)
        contract(2, k, left)
        send(3, k)
    lower, inverse = eliminate(lower, inverse, rank_one * 3 // 8, rank_one)
    basis_ref[...] = dot(inverse, image, ((1,), (0,)))
    inverse_high, inverse_low = split(inverse.T)
    weights = jnp.concatenate([inverse_high, inverse_high, inverse_low], axis=0)
    for k in range(copies):
        arrive(3, k)
    vectors = jnp.concatenate([collect(3, k) for k in range(copies)], axis=0)
    core = lax.dot_general(triple(vectors, 0), weights, (((0,), (0,)), ((), ())), preferred_element_type=jnp.float32)
    for c in range(local_three):
        for b in range(local_two):
            core_ref[b, c] = core[(c * local_two + b) * rank_four:(c * local_two + b + 1) * rank_four, :]

    for k in range(copies):
        for stage in range(4):
            wait_for(gots.at[stage, k, pl.ds(0, devices - 1)], send_sem.at[stage, k])
        wait_for(paired.at[k], share_sem.at[4, k])
        wait_for(shares.at[k], share_sem.at[0, k])
        wait_for(shares.at[k], share_sem.at[2, k])
        wait_for(paired.at[k], image_sem.at[0, k])
    wait_for(twos.at[pl.ds(0, rows - 1)], factor_sem.at[0])
    wait_for(threes.at[pl.ds(0, cols - 1)], factor_sem.at[2])


def write_kernel(core_ref, basis_ref, core_hbm, basis_hbm, sem):
    first = pltpu.make_async_copy(core_ref, core_hbm, sem.at[0])
    second = pltpu.make_async_copy(basis_ref, basis_hbm, sem.at[1])
    first.start()
    second.start()
    first.wait()
    second.wait()


def fits(tensor, factor_two, factor_three, factor_four, factor_init):
    rows, cols = lax.axis_size("row"), lax.axis_size("col")
    devices = rows * cols
    first_len, local_two, width = tensor.shape
    fourth_len, rank_four = factor_four.shape
    rank_one = factor_init.shape[1]
    local_three = width // fourth_len
    same = factor_two.shape[1] == local_two * rows and factor_three.shape[1] == local_three * cols
    even = rows % 2 == 0 and cols % 2 == 0 and rank_one % devices == 0
    flat = local_two * rank_four == LANES and width == LANES and (local_three == 4 or local_three % 8 == 0)
    tiles = (devices // 8) * (first_len // (2 * LANES))
    return same and even and flat and first_len % (4 * LANES) == 0 and devices % 8 == 0 and tiles == devices // 2


def fused(tensor, factor_two, factor_three, factor_four, factor_init):
    rows, cols = lax.axis_size("row"), lax.axis_size("col")
    devices = rows * cols
    members = devices // 2
    first_len, local_two, width = tensor.shape
    fourth_len, rank_four = factor_four.shape
    rank_one = factor_init.shape[1]
    local_three = width // fourth_len
    lanes = local_two * rank_four
    features = local_three * lanes
    total_width = local_two * width
    copies = rank_one // devices
    wide = rows * lanes

    def f32(*shape):
        return pltpu.VMEM(shape, jnp.float32)

    def bf16(*shape):
        return pltpu.VMEM(shape, jnp.bfloat16)

    vmem, hbm = pl.BlockSpec(memory_space=pltpu.VMEM), pl.BlockSpec(memory_space=pltpu.HBM)
    shapes = (
        jax.ShapeDtypeStruct((local_two, local_three, rank_four, rank_one), jnp.float32),
        jax.ShapeDtypeStruct((rank_one, first_len), jnp.float32),
    )
    operands = [pltpu.with_memory_space_constraint(x, pltpu.HBM) for x in (tensor, factor_two, factor_three, factor_four.T, factor_init.T)]
    core, basis = pl.pallas_call(
        hooi_kernel,
        out_shape=tuple(pltpu.VMEM(x.shape, x.dtype) for x in shapes),
        in_specs=[hbm] * 5,
        out_specs=(vmem, vmem),
        scratch_shapes=[
            f32(local_two, first_len, width), f32(*factor_two.shape), f32(*factor_three.shape), f32(rank_four, fourth_len), f32(rank_one, first_len),
            bf16(first_len, total_width), bf16(first_len, total_width), bf16(total_width, features), bf16(total_width, features),
            bf16(first_len, features), bf16(first_len, features), bf16(features, first_len), bf16(features, first_len),
            bf16(wide, wide), bf16(wide, wide), f32(rows, *factor_two.shape), f32(cols, *factor_three.shape),
            f32(4, copies, devices, local_three, lanes), f32(4, copies, devices, local_three, lanes),
            f32(copies, members, 8, LANES), f32(copies, members, 8, LANES), f32(copies, members, 8, LANES), f32(copies, members, 8, LANES),
            f32(copies, 8, LANES), f32(2, copies, members, 8, LANES),
            pltpu.SemaphoreType.DMA((local_two + 4,)),
            pltpu.SemaphoreType.DMA((4,)),
            pltpu.SemaphoreType.DMA((4, copies)),
            pltpu.SemaphoreType.DMA((4, copies)),
            pltpu.SemaphoreType.DMA((2, copies)),
            pltpu.SemaphoreType.DMA((6, copies)),
        ],
        compiler_params=pltpu.CompilerParams(collective_id=0, has_side_effects=True, vmem_limit_bytes=48 << 20),
    )(*operands)
    core, basis = pl.pallas_call(
        write_kernel,
        out_shape=shapes,
        in_specs=[vmem, vmem],
        out_specs=(hbm, hbm),
        scratch_shapes=[pltpu.SemaphoreType.DMA((2,))],
        compiler_params=pltpu.CompilerParams(vmem_limit_bytes=4 << 20),
    )(core, basis)
    return basis.T, core.transpose(3, 0, 1, 2)


def shards(tensor, factor_two, factor_three, factor_four, factor_init):
    if fits(tensor, factor_two, factor_three, factor_four, factor_init):
        return fused(tensor, factor_two, factor_three, factor_four, factor_init)
    axes = ("row", "col")
    first_len, local_two, width = tensor.shape
    fourth_len, rank_four = factor_four.shape
    local_three = width // fourth_len
    rank_one = factor_init.shape[1]
    rows, cols = lax.axis_size("row"), lax.axis_size("col")
    devices = rows * cols
    local_pairs = local_two * local_three
    features = rank_four * rank_one
    part = features // devices
    data = tensor.reshape(first_len, local_pairs, fourth_len)
    rank_two, rank_three = factor_two.shape[1], factor_three.shape[1]

    def pull(vectors):
        mixed = jnp.einsum("apd,ar->prd", data, vectors, precision=lax.Precision.HIGH)
        return jnp.einsum("prd,de->per", mixed, factor_four, precision=HIGHEST).reshape(local_pairs, features)

    def share(values, ident):
        length = values.shape[1]
        padded = -(-length // LANES) * LANES
        values = jnp.pad(values, ((0, 0), (0, padded - length))).reshape(devices, padded // LANES, LANES)
        return swap(values, ident).reshape(devices, padded)[:, :length]

    def spread(block, ident, extra=None):
        put = block.reshape(local_pairs, devices, part).transpose(1, 0, 2).reshape(devices, local_pairs * part)
        if extra is not None:
            put = jnp.concatenate([put, jnp.broadcast_to(extra[None], (devices, extra.shape[0]))], axis=1)
        got = share(put, ident)
        rest = got[:, local_pairs * part:]
        got = got[:, :local_pairs * part]
        got = got.reshape(rows, cols, local_two, local_three, part)
        return got.transpose(0, 2, 1, 3, 4).reshape(rows * local_two, cols * local_three, part), rest

    def gather(block, ident):
        two, three, _ = block.shape
        put = block.reshape(rows, two // rows, cols, three // cols, part).transpose(0, 2, 1, 3, 4)
        got = share(put.reshape(devices, -1), ident).reshape(devices, (two // rows) * (three // cols), part)
        return got.transpose(1, 0, 2).reshape(got.shape[1], features)

    extra = jnp.concatenate([factor_two.reshape(-1), factor_three.reshape(-1)])
    block, rest = spread(pull(factor_init), 1, extra)
    rest = rest.reshape(rows, cols, -1)
    whole_two = rest[:, 0, :factor_two.size].reshape(-1, rank_two)
    whole_three = rest[0, :, factor_two.size:].reshape(-1, rank_three)
    block = jnp.einsum("bcq,bg->gcq", block, whole_two, precision=HIGHEST)
    block = jnp.einsum("gcq,cf->gfq", block, whole_three, precision=HIGHEST)
    block = jnp.einsum("gfq,cf->gcq", block, whole_three, precision=HIGHEST)
    block = jnp.einsum("gcq,bg->bcq", block, whole_two, precision=HIGHEST)
    block = gather(block, 2).reshape(local_pairs, rank_four, rank_one)
    block = jnp.einsum("per,de->pdr", block, factor_four, precision=HIGHEST)
    image = jnp.dot(tensor.reshape(first_len, -1), block.reshape(-1, rank_one), precision=lax.Precision.HIGH)
    half = first_len // 2
    image = jnp.concatenate([image[:half], image[half:]], axis=1).reshape(devices, half // devices, 2 * rank_one)
    image = total(image, 0).reshape(half, 2 * rank_one)
    image = jnp.concatenate([image[:, :rank_one], image[:, rank_one:]], axis=0)
    basis, inverse = finish(image)
    block, _ = spread(pull(image), 3)
    block = jnp.einsum("bcq,bg->gcq", block, whole_two, precision=HIGHEST)
    block = jnp.einsum("gcq,cf->gfq", block, whole_three, precision=HIGHEST)
    block = gather(block, 4).reshape(-1, rank_four, rank_one)
    core = jnp.einsum("per,sr->spe", block, inverse, precision=HIGHEST)
    return (basis, core.reshape(rank_one, rank_two // rows, rank_three // cols, rank_four))


def solution(mesh):
    in_specs = (P(None, "row", "col"), P("row", None), P("col", None), P(), P())
    out_specs = (P(), P(None, "row", "col", None))
    return jax.shard_map(shards, mesh=mesh, in_specs=in_specs, out_specs=out_specs, check_vma=False)
```

```python
import functools

import jax
import jax.numpy as jnp
from jax import lax
from jax.experimental import pallas as pl
from jax.experimental.pallas import tpu as pltpu
from jax.sharding import PartitionSpec as P

HIGHEST = lax.Precision.HIGHEST
LANES = 128


def dot(a, b, dims):
    return lax.dot_general(a, b, (dims, ((), ())), precision=HIGHEST, preferred_element_type=jnp.float32)


def inverse_factor(square):
    size = square.shape[0]
    rows = lax.broadcasted_iota(jnp.int32, (size, size), 0)
    cols = lax.broadcasted_iota(jnp.int32, (size, size), 1)
    index = lax.broadcasted_iota(jnp.int32, (size, 1), 0)
    left = square
    right = jnp.where(rows == cols, 1.0, 0.0).astype(jnp.float32)
    for k in range(size):
        scale = lax.rsqrt(left[k:k + 1, k:k + 1])
        column = left[:, k:k + 1] * scale
        pivot_left = left[k:k + 1, :] * scale
        pivot_right = right[k:k + 1, :] * scale
        factor = jnp.where(index > k, column, 0.0)
        left = left - factor * pivot_left
        right = jnp.where(index == k, pivot_right, right - factor * pivot_right)
    return right


def finish_kernel(image_ref, basis_ref, inverse_ref):
    image = image_ref[...]
    inverse = inverse_factor(dot(image, image, ((0,), (0,))))
    inverse_ref[...] = inverse
    basis_ref[...] = dot(image, inverse, ((1,), (1,)))


def finish(image):
    rank = image.shape[1]
    return pl.pallas_call(
        finish_kernel,
        out_shape=(
            jax.ShapeDtypeStruct(image.shape, jnp.float32),
            jax.ShapeDtypeStruct((rank, rank), jnp.float32),
        ),
    )(image)


def place():
    return lax.axis_index("row") * lax.axis_size("col") + lax.axis_index("col")


def greet(devices):
    cols = lax.axis_size("col")
    me = place()
    barrier = pltpu.get_barrier_semaphore()

    def hello(k, carry):
        peer = lax.rem(me + k, devices)
        pl.semaphore_signal(barrier, inc=1, device_id=(peer // cols, lax.rem(peer, cols)), device_id_type=pl.DeviceIdType.MESH)
        return carry

    lax.fori_loop(1, devices, hello, 0)
    pl.semaphore_wait(barrier, devices - 1)


def send_all(devices, source, target, send_sem, recv_sem):
    cols = lax.axis_size("col")
    me = place()

    def send(k, carry):
        peer = lax.rem(me + k, devices)
        pltpu.make_async_remote_copy(
            src_ref=source(peer),
            dst_ref=target.at[me],
            send_sem=send_sem,
            recv_sem=recv_sem,
            device_id=(peer // cols, lax.rem(peer, cols)),
            device_id_type=pl.DeviceIdType.MESH,
        ).start()
        return carry

    lax.fori_loop(1, devices, send, 0)
    whole = target.at[pl.ds(0, devices - 1)]
    pltpu.make_async_copy(whole, whole, send_sem).wait()
    pltpu.make_async_copy(whole, whole, recv_sem).wait()


def swap_kernel(devices, put_ref, out_ref, held, send_sem, recv_sem):
    me = place()
    greet(devices)
    send_all(devices, lambda peer: put_ref.at[peer], held, send_sem, recv_sem)
    held[me] = put_ref[me]
    out_ref[...] = held[...]


def total_kernel(devices, put_ref, out_ref, held, mine, spread, sems):
    me = place()
    greet(devices)
    send_all(devices, lambda peer: put_ref.at[peer], held, sems.at[0], sems.at[1])
    held[me] = put_ref[me]
    mine[...] = jnp.sum(held[...], axis=0)
    send_all(devices, lambda peer: mine, spread, sems.at[2], sems.at[3])
    spread[me] = mine[...]
    out_ref[...] = spread[...]


def swap(values, ident):
    devices = values.shape[0]
    return pl.pallas_call(
        functools.partial(swap_kernel, devices),
        out_shape=jax.ShapeDtypeStruct(values.shape, jnp.float32),
        in_specs=[pl.BlockSpec(memory_space=pltpu.VMEM)],
        out_specs=pl.BlockSpec(memory_space=pltpu.VMEM),
        scratch_shapes=[pltpu.VMEM(values.shape, jnp.float32), pltpu.SemaphoreType.DMA, pltpu.SemaphoreType.DMA],
        compiler_params=pltpu.CompilerParams(collective_id=ident, has_side_effects=True),
    )(values)


def total(values, ident):
    devices = values.shape[0]
    return pl.pallas_call(
        functools.partial(total_kernel, devices),
        out_shape=jax.ShapeDtypeStruct(values.shape, jnp.float32),
        in_specs=[pl.BlockSpec(memory_space=pltpu.VMEM)],
        out_specs=pl.BlockSpec(memory_space=pltpu.VMEM),
        scratch_shapes=[
            pltpu.VMEM(values.shape, jnp.float32),
            pltpu.VMEM(values.shape[1:], jnp.float32),
            pltpu.VMEM(values.shape, jnp.float32),
            pltpu.SemaphoreType.DMA((4,)),
        ],
        compiler_params=pltpu.CompilerParams(collective_id=ident, has_side_effects=True),
    )(values)


def split(x):
    high = x.astype(jnp.bfloat16)
    return high, (x - high.astype(jnp.float32)).astype(jnp.bfloat16)


def narrow(a, b):
    return lax.dot_general(a, b, (((1,), (0,)), ((), ())), preferred_element_type=jnp.float32)


def left_split(x, high, low):
    rows = x.shape[0]
    top, rest = split(x)
    both = narrow(jnp.concatenate([top, rest], axis=0), high)
    return both[:rows] + both[rows:] + narrow(top, low)


def iota(shape, dim):
    return lax.broadcasted_iota(jnp.int32, shape, dim)


def ones_where(mask):
    return jnp.where(mask, 1.0, 0.0).astype(jnp.float32)


def store_lanes(matrix, copies, high_ref, low_ref):
    shape = (matrix.shape[1], matrix.shape[1] * copies)
    wide = dot(matrix, ones_where(iota(shape, 1) // copies == iota(shape, 0)), ((1,), (0,)))
    shape = (copies, shape[1])
    keep = iota(shape, 1) % copies == iota(shape, 0)
    for k in range(matrix.shape[0]):
        high, low = split(jnp.where(keep, jnp.broadcast_to(wide[k:k + 1, :], shape), 0.0))
        high_ref[k * copies:(k + 1) * copies, :] = high
        low_ref[k * copies:(k + 1) * copies, :] = low


def eliminate(left, right, first, last):
    size = left.shape[0]
    index = iota((size, 1), 0)
    for k in range(first, last):
        scale = lax.rsqrt(left[k:k + 1, k:k + 1])
        column = left[:, k:k + 1] * scale
        pivot_left = left[k:k + 1, :] * scale
        pivot_right = right[k:k + 1, :] * scale
        factor = jnp.where(index > k, column, 0.0)
        left = left - factor * pivot_left
        right = jnp.where(index == k, pivot_right, right - factor * pivot_right)
    return left, right


def copy_to(source, target, row, col, send_sem, recv_sem):
    pltpu.make_async_remote_copy(
        src_ref=source,
        dst_ref=target,
        send_sem=send_sem,
        recv_sem=recv_sem,
        device_id=(row, col),
        device_id_type=pl.DeviceIdType.MESH,
    ).start()


def wait_for(ref, sem):
    pltpu.make_async_copy(ref, ref, sem).wait()


def hooi_kernel(tensor_hbm, two_hbm, three_hbm, four_hbm, init_hbm, core_ref, basis_ref,
                slabs, two_ref, three_ref, four_ref, init_ref,
                high_ref, low_ref, mix_high, mix_low, hat_high, hat_low, turn_high, turn_low,
                lane_high, lane_low, twos, threes, puts, gots,
                parts, paired, sums, shares, mine, spread,
                load_sem, factor_sem, send_sem, recv_sem, image_sem, share_sem):
    rows, cols = lax.axis_size("row"), lax.axis_size("col")
    row, col = lax.axis_index("row"), lax.axis_index("col")
    devices = rows * cols
    members = devices // 2
    half = lax.rem(row, 2)
    seat = (row // 2) * cols + col
    me = row * cols + col
    partner = row + 1 - 2 * half
    rank_one, first_len = init_ref.shape
    half_len = first_len // 2
    local_two, local_three = two_ref.shape[0], three_ref.shape[0]
    rank_four, fourth_len = four_ref.shape
    width = local_three * fourth_len
    lanes = local_two * rank_four
    features = local_three * lanes
    copies = rank_one // devices
    spans = half_len // LANES

    slab_loads = [pltpu.make_async_copy(tensor_hbm.at[:, b, :], slabs.at[b], load_sem.at[b]) for b in range(local_two)]
    small = [(four_hbm, four_ref), (init_hbm, init_ref), (two_hbm, two_ref), (three_hbm, three_ref)]
    small_loads = [pltpu.make_async_copy(source, target, load_sem.at[local_two + k]) for k, (source, target) in enumerate(small)]
    small_loads[0].start()
    small_loads[1].start()
    for load in slab_loads:
        load.start()
    small_loads[2].start()
    small_loads[3].start()

    pairs = cols // 2
    turns = sorted(range(pairs), key=lambda z: (z == 0, -abs(2 * z - pairs)))
    away = [d for d in [(near, far, flip) for flip in (1, 0) for near in reversed(range(rows // 2)) for far in turns] if any(d)]

    def there(distance):
        near, far, flip = distance
        return lax.rem(row // 2 + near, rows // 2), lax.rem(col // 2 + far, pairs) * 2 + lax.rem(col + flip, 2)

    def at(index, count):
        return pl.ds(pl.multiple_of(index * count, count), count)

    barrier = pltpu.get_barrier_semaphore()

    def greet_at(there_row, there_col):
        pl.semaphore_signal(barrier, inc=1, device_id=(there_row, there_col), device_id_type=pl.DeviceIdType.MESH)

    for distance in away:
        there_row, there_col = there(distance)
        greet_at(there_row * 2, there_col)
        greet_at(there_row * 2 + 1, there_col)
    greet_at(partner, col)

    small_loads[0].wait()
    lane = iota((fourth_len, features), 1)
    shape = (rank_four, features)
    four = dot(four_ref[...], ones_where(iota(shape, 1) % rank_four == iota(shape, 0)), ((0,), (0,)))
    four_high = four.astype(jnp.bfloat16).astype(jnp.float32)
    four_low = four - four_high
    for b in range(local_two):
        for c in range(local_three):
            keep = lane // rank_four == c * local_two + b
            part = slice((b * local_three + c) * fourth_len, (b * local_three + c + 1) * fourth_len)
            mix_high[part, :] = jnp.where(keep, four_high, 0.0).astype(jnp.bfloat16)
            mix_low[part, :] = jnp.where(keep, four_low, 0.0).astype(jnp.bfloat16)

    small_loads[1].wait()
    init_high, init_low = split(init_ref[...])
    init_both = jnp.concatenate([init_high, init_low], axis=0)
    cuts = [0, local_two // 2, local_two]
    count = len(cuts) - 1

    def span_of(k):
        return slice(cuts[k] * width, cuts[k + 1] * width)

    def pull_group(k):
        both = narrow(init_both, high_ref[:, span_of(k)])
        return both[:rank_one] + both[rank_one:] + narrow(init_high, low_ref[:, span_of(k)])

    pulled, vectors = [], []
    for k in range(count + 2):
        if k < count:
            for b in range(cuts[k], cuts[k + 1]):
                slab_loads[b].wait()
                high, low = split(slabs[b])
                high_ref[:, b * width:(b + 1) * width] = high
                low_ref[:, b * width:(b + 1) * width] = low
        if k >= 2:
            vectors.append(left_split(pulled[k - 2], mix_high[span_of(k - 2), :], mix_low[span_of(k - 2), :]))
        if 1 <= k <= count:
            pulled.append(pull_group(k - 1))
    vectors = sum(vectors[1:], vectors[0])

    def fenced(body):
        def trip(_, carry):
            body()
            return carry

        lax.fori_loop(0, 1 + me // devices, trip, 0)

    def flat(ref):
        return ref.reshape(devices * local_three, lanes)

    def deal(vectors, put):
        for c in range(local_three):
            put[pl.ds(c, devices, stride=local_three), :] = vectors[:, c * lanes:(c + 1) * lanes]

    def send(stage, k):
        put, got = puts.at[stage, k], gots.at[stage, k]

        def one(there_row, there_col):
            copy_to(put.at[there_row * cols + there_col], got.at[me], there_row, there_col, send_sem.at[stage, k], recv_sem.at[stage, k])

        @fenced
        def _():
            for h in range(2):
                for distance in away:
                    there_row, there_col = there(distance)
                    one(there_row * 2 + h, there_col)
            one(partner, col)

        got[me] = put[me]

    def arrive(stage, k):
        wait_for(gots.at[stage, k, pl.ds(0, devices - 1)], recv_sem.at[stage, k])

    def contract(stage, k, matrix):
        got, put = flat(gots.at[stage, k]), flat(puts.at[stage + 1, k])
        size = cols * local_three
        top, rest = split(jnp.concatenate([got[i * size:(i + 1) * size, :] for i in range(rows)], axis=1))
        result = left_split(narrow(matrix, jnp.concatenate([top, top, rest], axis=0)), lane_high[...], lane_low[...])
        for i in range(rows):
            put[i * size:(i + 1) * size, :] = result[:, i * lanes:(i + 1) * lanes]

    def triple(matrix, axis):
        high, low = split(matrix)
        return jnp.concatenate([high, low, high], axis=axis)

    def collect(stage, k):
        got = flat(gots.at[stage, k])
        return jnp.concatenate([got[pl.ds(c, devices, stride=local_three), :] for c in range(local_three)], axis=1)

    for k in range(copies):
        deal(vectors[k * devices:(k + 1) * devices], flat(puts.at[0, k]))
    small_loads[2].wait()
    small_loads[3].wait()
    pl.semaphore_wait(barrier, devices - 1)

    def send_two(k, carry):
        copy_to(two_ref, twos.at[row], lax.rem(row + k, rows), col, factor_sem.at[0], factor_sem.at[1])
        return carry

    def send_three(k, carry):
        copy_to(three_ref, threes.at[col], row, lax.rem(col + k, cols), factor_sem.at[2], factor_sem.at[3])
        return carry

    lax.fori_loop(1, rows, send_two, 0, unroll=True)
    lax.fori_loop(1, cols, send_three, 0, unroll=True)
    for k in range(copies):
        send(0, k)
    twos[row] = two_ref[...]
    threes[col] = three_ref[...]

    def hat_piece(k, count):
        part = slice(k * first_len // count, (k + 1) * first_len // count)
        hat = narrow(high_ref[part, :], mix_high[...]) + narrow(high_ref[part, :], mix_low[...]) + narrow(low_ref[part, :], mix_high[...])
        hat_high[part, :], hat_low[part, :] = split(hat)
        turn_high[:, part], turn_low[:, part] = split(hat.T)

    hat_piece(0, 4)
    wait_for(twos.at[pl.ds(0, rows - 1)], factor_sem.at[1])
    wait_for(threes.at[pl.ds(0, cols - 1)], factor_sem.at[3])
    whole_two = jnp.concatenate([twos[k] for k in range(rows)], axis=0)
    whole_three = jnp.concatenate([threes[k] for k in range(cols)], axis=0)
    store_lanes(dot(whole_two, whole_two, ((1,), (1,))), rank_four, lane_high, lane_low)
    left = triple(dot(whole_three, whole_three, ((1,), (1,))), 1)

    for k in range(copies):
        arrive(0, k)
        contract(0, k, left)
        send(1, k)
    hat_piece(1, 4)
    hat_piece(2, 4)
    hat_piece(3, 4)

    def tiles():
        for i in range(members):
            r, w = i // spans, i % spans
            yield i, slice(r * 8, (r + 1) * 8), slice(w * LANES, (w + 1) * LANES)

    def image_part(back, which):
        span = at(which, half_len)
        return left_split(back, turn_high[:, span], turn_low[:, span])

    def image_out(k):
        back = collect(1, k)
        image = image_part(back, 1 - half)
        for i, r, w in tiles():
            parts[k, i] = image[r, w]
        fenced(lambda: copy_to(parts.at[k], paired.at[k], partner, col, share_sem.at[4, k], share_sem.at[5, k]))
        return back

    def scatter(k, image):
        wait_for(paired.at[k], share_sem.at[5, k])
        for i, r, w in tiles():
            sums[k, i] = image[r, w] + paired[k, i]

        @fenced
        def _():
            for distance in away + [(0, 0, 0)]:
                there_row, there_col = there(distance)
                copy_to(sums.at[k, there_row * cols + there_col], shares.at[k, seat], there_row * 2 + 1 - half, there_col, share_sem.at[0, k], share_sem.at[1, k])

    arrive(1, 0)
    owned = image_part(image_out(0), half)
    for k in range(copies):
        if k + 1 < copies:
            arrive(1, k + 1)
            back = image_out(k + 1)
        scatter(k, owned)
        if k + 1 < copies:
            owned = image_part(back, half)

    store_lanes(whole_two, rank_four, lane_high, lane_low)
    left = triple(whole_three.T, 1)
    for k in range(copies):
        wait_for(shares.at[k], share_sem.at[1, k])
        mine[k] = jnp.sum(shares[k], axis=0)

        @fenced
        def _():
            for distance in away + [(0, 0, 0)]:
                there_row, there_col = there(distance)
                copy_to(mine.at[k], spread.at[1 - half, k, seat], there_row * 2 + 1 - half, there_col, share_sem.at[2, k], share_sem.at[3, k])

    def image_half(which, k):
        return jnp.concatenate([
            jnp.concatenate([spread[which, k, r * spans + w] for w in range(spans)], axis=1)
            for r in range(members // spans)], axis=0)

    def pull_half(which, k):
        span = at(which, half_len)
        return left_split(image_half(which, k), hat_high[span, :], hat_low[span, :])

    def pass_on(k):
        wait_for(spread.at[half, k], share_sem.at[3, k])
        fenced(lambda: copy_to(spread.at[half, k], spread.at[half, k], partner, col, image_sem.at[0, k], image_sem.at[1, k]))

    pass_on(0)
    for k in range(copies):
        vectors = pull_half(half, k)
        if k + 1 < copies:
            pass_on(k + 1)
        wait_for(spread.at[1 - half, k], image_sem.at[1, k])
        deal(vectors + pull_half(1 - half, k), flat(puts.at[2, k]))
        send(2, k)

    image = jnp.concatenate([jnp.concatenate([image_half(0, k), image_half(1, k)], axis=1) for k in range(copies)], axis=0)
    lower = dot(image, image, ((1,), (1,)))
    shape = lower.shape
    lower, inverse = eliminate(lower, ones_where(iota(shape, 0) == iota(shape, 1)), 0, rank_one * 3 // 8)
    for k in range(copies):
        arrive(2, k)
        contract(2, k, left)
        send(3, k)
    lower, inverse = eliminate(lower, inverse, rank_one * 3 // 8, rank_one)
    basis_ref[...] = dot(inverse, image, ((1,), (0,)))
    inverse_high, inverse_low = split(inverse.T)
    core = None
    for k in range(copies):
        arrive(3, k)
        part = slice(k * devices, (k + 1) * devices)
        weights = jnp.concatenate([inverse_high[part], inverse_high[part], inverse_low[part]], axis=0)
        more = lax.dot_general(triple(collect(3, k), 0), weights, (((0,), (0,)), ((), ())), preferred_element_type=jnp.float32)
        core = more if core is None else core + more
    for c in range(local_three):
        for b in range(local_two):
            core_ref[b, c] = core[(c * local_two + b) * rank_four:(c * local_two + b + 1) * rank_four, :]

    for k in range(copies):
        for stage in range(4):
            wait_for(gots.at[stage, k, pl.ds(0, devices - 1)], send_sem.at[stage, k])
        wait_for(paired.at[k], share_sem.at[4, k])
        wait_for(shares.at[k], share_sem.at[0, k])
        wait_for(shares.at[k], share_sem.at[2, k])
        wait_for(paired.at[k], image_sem.at[0, k])
    wait_for(twos.at[pl.ds(0, rows - 1)], factor_sem.at[0])
    wait_for(threes.at[pl.ds(0, cols - 1)], factor_sem.at[2])


def write_kernel(core_ref, basis_ref, core_hbm, basis_hbm, sem):
    first = pltpu.make_async_copy(core_ref, core_hbm, sem.at[0])
    second = pltpu.make_async_copy(basis_ref, basis_hbm, sem.at[1])
    first.start()
    second.start()
    first.wait()
    second.wait()


def fits(tensor, factor_two, factor_three, factor_four, factor_init):
    rows, cols = lax.axis_size("row"), lax.axis_size("col")
    devices = rows * cols
    first_len, local_two, width = tensor.shape
    fourth_len, rank_four = factor_four.shape
    rank_one = factor_init.shape[1]
    local_three = width // fourth_len
    same = factor_two.shape[1] == local_two * rows and factor_three.shape[1] == local_three * cols
    even = rows % 2 == 0 and cols % 2 == 0 and rank_one % devices == 0
    flat = local_two * rank_four == LANES and width == LANES and (local_three == 4 or local_three % 8 == 0)
    tiles = (devices // 8) * (first_len // (2 * LANES))
    return same and even and flat and first_len % (4 * LANES) == 0 and devices % 8 == 0 and tiles == devices // 2


def fused(tensor, factor_two, factor_three, factor_four, factor_init):
    rows, cols = lax.axis_size("row"), lax.axis_size("col")
    devices = rows * cols
    members = devices // 2
    first_len, local_two, width = tensor.shape
    fourth_len, rank_four = factor_four.shape
    rank_one = factor_init.shape[1]
    local_three = width // fourth_len
    lanes = local_two * rank_four
    features = local_three * lanes
    total_width = local_two * width
    copies = rank_one // devices
    wide = rows * lanes

    def f32(*shape):
        return pltpu.VMEM(shape, jnp.float32)

    def bf16(*shape):
        return pltpu.VMEM(shape, jnp.bfloat16)

    vmem, hbm = pl.BlockSpec(memory_space=pltpu.VMEM), pl.BlockSpec(memory_space=pltpu.HBM)
    shapes = (
        jax.ShapeDtypeStruct((local_two, local_three, rank_four, rank_one), jnp.float32),
        jax.ShapeDtypeStruct((rank_one, first_len), jnp.float32),
    )
    operands = [pltpu.with_memory_space_constraint(x, pltpu.HBM) for x in (tensor, factor_two, factor_three, factor_four.T, factor_init.T)]
    core, basis = pl.pallas_call(
        hooi_kernel,
        out_shape=tuple(pltpu.VMEM(x.shape, x.dtype) for x in shapes),
        in_specs=[hbm] * 5,
        out_specs=(vmem, vmem),
        scratch_shapes=[
            f32(local_two, first_len, width), f32(*factor_two.shape), f32(*factor_three.shape), f32(rank_four, fourth_len), f32(rank_one, first_len),
            bf16(first_len, total_width), bf16(first_len, total_width), bf16(total_width, features), bf16(total_width, features),
            bf16(first_len, features), bf16(first_len, features), bf16(features, first_len), bf16(features, first_len),
            bf16(wide, wide), bf16(wide, wide), f32(rows, *factor_two.shape), f32(cols, *factor_three.shape),
            f32(4, copies, devices, local_three, lanes), f32(4, copies, devices, local_three, lanes),
            f32(copies, members, 8, LANES), f32(copies, members, 8, LANES), f32(copies, members, 8, LANES), f32(copies, members, 8, LANES),
            f32(copies, 8, LANES), f32(2, copies, members, 8, LANES),
            pltpu.SemaphoreType.DMA((local_two + 4,)),
            pltpu.SemaphoreType.DMA((4,)),
            pltpu.SemaphoreType.DMA((4, copies)),
            pltpu.SemaphoreType.DMA((4, copies)),
            pltpu.SemaphoreType.DMA((2, copies)),
            pltpu.SemaphoreType.DMA((6, copies)),
        ],
        compiler_params=pltpu.CompilerParams(collective_id=0, has_side_effects=True, vmem_limit_bytes=48 << 20),
    )(*operands)
    core, basis = pl.pallas_call(
        write_kernel,
        out_shape=shapes,
        in_specs=[vmem, vmem],
        out_specs=(hbm, hbm),
        scratch_shapes=[pltpu.SemaphoreType.DMA((2,))],
        compiler_params=pltpu.CompilerParams(vmem_limit_bytes=4 << 20),
    )(core, basis)
    return basis.T, core.transpose(3, 0, 1, 2)


def shards(tensor, factor_two, factor_three, factor_four, factor_init):
    if fits(tensor, factor_two, factor_three, factor_four, factor_init):
        return fused(tensor, factor_two, factor_three, factor_four, factor_init)
    axes = ("row", "col")
    first_len, local_two, width = tensor.shape
    fourth_len, rank_four = factor_four.shape
    local_three = width // fourth_len
    rank_one = factor_init.shape[1]
    rows, cols = lax.axis_size("row"), lax.axis_size("col")
    devices = rows * cols
    local_pairs = local_two * local_three
    features = rank_four * rank_one
    part = features // devices
    data = tensor.reshape(first_len, local_pairs, fourth_len)
    rank_two, rank_three = factor_two.shape[1], factor_three.shape[1]

    def pull(vectors):
        mixed = jnp.einsum("apd,ar->prd", data, vectors, precision=lax.Precision.HIGH)
        return jnp.einsum("prd,de->per", mixed, factor_four, precision=HIGHEST).reshape(local_pairs, features)

    def share(values, ident):
        length = values.shape[1]
        padded = -(-length // LANES) * LANES
        values = jnp.pad(values, ((0, 0), (0, padded - length))).reshape(devices, padded // LANES, LANES)
        return swap(values, ident).reshape(devices, padded)[:, :length]

    def spread(block, ident, extra=None):
        put = block.reshape(local_pairs, devices, part).transpose(1, 0, 2).reshape(devices, local_pairs * part)
        if extra is not None:
            put = jnp.concatenate([put, jnp.broadcast_to(extra[None], (devices, extra.shape[0]))], axis=1)
        got = share(put, ident)
        rest = got[:, local_pairs * part:]
        got = got[:, :local_pairs * part]
        got = got.reshape(rows, cols, local_two, local_three, part)
        return got.transpose(0, 2, 1, 3, 4).reshape(rows * local_two, cols * local_three, part), rest

    def gather(block, ident):
        two, three, _ = block.shape
        put = block.reshape(rows, two // rows, cols, three // cols, part).transpose(0, 2, 1, 3, 4)
        got = share(put.reshape(devices, -1), ident).reshape(devices, (two // rows) * (three // cols), part)
        return got.transpose(1, 0, 2).reshape(got.shape[1], features)

    extra = jnp.concatenate([factor_two.reshape(-1), factor_three.reshape(-1)])
    block, rest = spread(pull(factor_init), 1, extra)
    rest = rest.reshape(rows, cols, -1)
    whole_two = rest[:, 0, :factor_two.size].reshape(-1, rank_two)
    whole_three = rest[0, :, factor_two.size:].reshape(-1, rank_three)
    block = jnp.einsum("bcq,bg->gcq", block, whole_two, precision=HIGHEST)
    block = jnp.einsum("gcq,cf->gfq", block, whole_three, precision=HIGHEST)
    block = jnp.einsum("gfq,cf->gcq", block, whole_three, precision=HIGHEST)
    block = jnp.einsum("gcq,bg->bcq", block, whole_two, precision=HIGHEST)
    block = gather(block, 2).reshape(local_pairs, rank_four, rank_one)
    block = jnp.einsum("per,de->pdr", block, factor_four, precision=HIGHEST)
    image = jnp.dot(tensor.reshape(first_len, -1), block.reshape(-1, rank_one), precision=lax.Precision.HIGH)
    half = first_len // 2
    image = jnp.concatenate([image[:half], image[half:]], axis=1).reshape(devices, half // devices, 2 * rank_one)
    image = total(image, 0).reshape(half, 2 * rank_one)
    image = jnp.concatenate([image[:, :rank_one], image[:, rank_one:]], axis=0)
    basis, inverse = finish(image)
    block, _ = spread(pull(image), 3)
    block = jnp.einsum("bcq,bg->gcq", block, whole_two, precision=HIGHEST)
    block = jnp.einsum("gcq,cf->gfq", block, whole_three, precision=HIGHEST)
    block = gather(block, 4).reshape(-1, rank_four, rank_one)
    core = jnp.einsum("per,sr->spe", block, inverse, precision=HIGHEST)
    return (basis, core.reshape(rank_one, rank_two // rows, rank_three // cols, rank_four))


def solution(mesh):
    in_specs = (P(None, "row", "col"), P("row", None), P("col", None), P(), P())
    out_specs = (P(), P(None, "row", "col", None))
    return jax.shard_map(shards, mesh=mesh, in_specs=in_specs, out_specs=out_specs, check_vma=False)
```

```python
import functools

import jax
import jax.numpy as jnp
from jax import lax
from jax.experimental import pallas as pl
from jax.experimental.pallas import tpu as pltpu
from jax.sharding import PartitionSpec as P

HIGHEST = lax.Precision.HIGHEST
LANES = 128


def dot(a, b, dims):
    return lax.dot_general(a, b, (dims, ((), ())), precision=HIGHEST, preferred_element_type=jnp.float32)


def inverse_factor(square):
    size = square.shape[0]
    rows = lax.broadcasted_iota(jnp.int32, (size, size), 0)
    cols = lax.broadcasted_iota(jnp.int32, (size, size), 1)
    index = lax.broadcasted_iota(jnp.int32, (size, 1), 0)
    left = square
    right = jnp.where(rows == cols, 1.0, 0.0).astype(jnp.float32)
    for k in range(size):
        scale = lax.rsqrt(left[k:k + 1, k:k + 1])
        column = left[:, k:k + 1] * scale
        pivot_left = left[k:k + 1, :] * scale
        pivot_right = right[k:k + 1, :] * scale
        factor = jnp.where(index > k, column, 0.0)
        left = left - factor * pivot_left
        right = jnp.where(index == k, pivot_right, right - factor * pivot_right)
    return right


def finish_kernel(image_ref, basis_ref, inverse_ref):
    image = image_ref[...]
    inverse = inverse_factor(dot(image, image, ((0,), (0,))))
    inverse_ref[...] = inverse
    basis_ref[...] = dot(image, inverse, ((1,), (1,)))


def finish(image):
    rank = image.shape[1]
    return pl.pallas_call(
        finish_kernel,
        out_shape=(
            jax.ShapeDtypeStruct(image.shape, jnp.float32),
            jax.ShapeDtypeStruct((rank, rank), jnp.float32),
        ),
    )(image)


def place():
    return lax.axis_index("row") * lax.axis_size("col") + lax.axis_index("col")


def greet(devices):
    cols = lax.axis_size("col")
    me = place()
    barrier = pltpu.get_barrier_semaphore()

    def hello(k, carry):
        peer = lax.rem(me + k, devices)
        pl.semaphore_signal(barrier, inc=1, device_id=(peer // cols, lax.rem(peer, cols)), device_id_type=pl.DeviceIdType.MESH)
        return carry

    lax.fori_loop(1, devices, hello, 0)
    pl.semaphore_wait(barrier, devices - 1)


def send_all(devices, source, target, send_sem, recv_sem):
    cols = lax.axis_size("col")
    me = place()

    def send(k, carry):
        peer = lax.rem(me + k, devices)
        pltpu.make_async_remote_copy(
            src_ref=source(peer),
            dst_ref=target.at[me],
            send_sem=send_sem,
            recv_sem=recv_sem,
            device_id=(peer // cols, lax.rem(peer, cols)),
            device_id_type=pl.DeviceIdType.MESH,
        ).start()
        return carry

    lax.fori_loop(1, devices, send, 0)
    whole = target.at[pl.ds(0, devices - 1)]
    pltpu.make_async_copy(whole, whole, send_sem).wait()
    pltpu.make_async_copy(whole, whole, recv_sem).wait()


def swap_kernel(devices, put_ref, out_ref, held, send_sem, recv_sem):
    me = place()
    greet(devices)
    send_all(devices, lambda peer: put_ref.at[peer], held, send_sem, recv_sem)
    held[me] = put_ref[me]
    out_ref[...] = held[...]


def total_kernel(devices, put_ref, out_ref, held, mine, spread, sems):
    me = place()
    greet(devices)
    send_all(devices, lambda peer: put_ref.at[peer], held, sems.at[0], sems.at[1])
    held[me] = put_ref[me]
    mine[...] = jnp.sum(held[...], axis=0)
    send_all(devices, lambda peer: mine, spread, sems.at[2], sems.at[3])
    spread[me] = mine[...]
    out_ref[...] = spread[...]


def swap(values, ident):
    devices = values.shape[0]
    return pl.pallas_call(
        functools.partial(swap_kernel, devices),
        out_shape=jax.ShapeDtypeStruct(values.shape, jnp.float32),
        in_specs=[pl.BlockSpec(memory_space=pltpu.VMEM)],
        out_specs=pl.BlockSpec(memory_space=pltpu.VMEM),
        scratch_shapes=[pltpu.VMEM(values.shape, jnp.float32), pltpu.SemaphoreType.DMA, pltpu.SemaphoreType.DMA],
        compiler_params=pltpu.CompilerParams(collective_id=ident, has_side_effects=True),
    )(values)


def total(values, ident):
    devices = values.shape[0]
    return pl.pallas_call(
        functools.partial(total_kernel, devices),
        out_shape=jax.ShapeDtypeStruct(values.shape, jnp.float32),
        in_specs=[pl.BlockSpec(memory_space=pltpu.VMEM)],
        out_specs=pl.BlockSpec(memory_space=pltpu.VMEM),
        scratch_shapes=[
            pltpu.VMEM(values.shape, jnp.float32),
            pltpu.VMEM(values.shape[1:], jnp.float32),
            pltpu.VMEM(values.shape, jnp.float32),
            pltpu.SemaphoreType.DMA((4,)),
        ],
        compiler_params=pltpu.CompilerParams(collective_id=ident, has_side_effects=True),
    )(values)


def split(x):
    high = x.astype(jnp.bfloat16)
    return high, (x - high.astype(jnp.float32)).astype(jnp.bfloat16)


def narrow(a, b):
    return lax.dot_general(a, b, (((1,), (0,)), ((), ())), preferred_element_type=jnp.float32)


def left_split(x, high, low):
    rows = x.shape[0]
    top, rest = split(x)
    both = narrow(jnp.concatenate([top, rest], axis=0), high)
    return both[:rows] + both[rows:] + narrow(top, low)


def iota(shape, dim):
    return lax.broadcasted_iota(jnp.int32, shape, dim)


def ones_where(mask):
    return jnp.where(mask, 1.0, 0.0).astype(jnp.float32)


def store_lanes(matrix, copies, high_ref, low_ref):
    shape = (matrix.shape[1], matrix.shape[1] * copies)
    wide = dot(matrix, ones_where(iota(shape, 1) // copies == iota(shape, 0)), ((1,), (0,)))
    shape = (copies, shape[1])
    keep = iota(shape, 1) % copies == iota(shape, 0)
    for k in range(matrix.shape[0]):
        high, low = split(jnp.where(keep, jnp.broadcast_to(wide[k:k + 1, :], shape), 0.0))
        high_ref[k * copies:(k + 1) * copies, :] = high
        low_ref[k * copies:(k + 1) * copies, :] = low


def eliminate(left, right, first, last):
    size = left.shape[0]
    index = iota((size, 1), 0)
    for k in range(first, last):
        scale = lax.rsqrt(left[k:k + 1, k:k + 1])
        column = left[:, k:k + 1] * scale
        pivot_left = left[k:k + 1, :] * scale
        pivot_right = right[k:k + 1, :] * scale
        factor = jnp.where(index > k, column, 0.0)
        left = left - factor * pivot_left
        right = jnp.where(index == k, pivot_right, right - factor * pivot_right)
    return left, right


def copy_to(source, target, row, col, send_sem, recv_sem):
    pltpu.make_async_remote_copy(
        src_ref=source,
        dst_ref=target,
        send_sem=send_sem,
        recv_sem=recv_sem,
        device_id=(row, col),
        device_id_type=pl.DeviceIdType.MESH,
    ).start()


def wait_for(ref, sem):
    pltpu.make_async_copy(ref, ref, sem).wait()


def hooi_kernel(tensor_hbm, two_hbm, three_hbm, four_hbm, init_hbm, core_ref, basis_ref,
                slabs, two_ref, three_ref, four_ref, init_ref,
                high_ref, low_ref, mix_high, mix_low, hat_high, hat_low, turn_high, turn_low,
                lane_high, lane_low, twos, threes, puts, gots,
                parts, paired, sums, shares, mine, spread,
                load_sem, factor_sem, send_sem, recv_sem, image_sem, share_sem):
    rows, cols = lax.axis_size("row"), lax.axis_size("col")
    row, col = lax.axis_index("row"), lax.axis_index("col")
    devices = rows * cols
    members = devices // 2
    half = lax.rem(row, 2)
    seat = (row // 2) * cols + col
    me = row * cols + col
    partner = row + 1 - 2 * half
    rank_one, first_len = init_ref.shape
    half_len = first_len // 2
    local_two, local_three = two_ref.shape[0], three_ref.shape[0]
    rank_four, fourth_len = four_ref.shape
    width = local_three * fourth_len
    lanes = local_two * rank_four
    features = local_three * lanes
    copies = rank_one // devices
    spans = half_len // LANES

    slab_loads = [pltpu.make_async_copy(tensor_hbm.at[:, b, :], slabs.at[b], load_sem.at[b]) for b in range(local_two)]
    small = [(four_hbm, four_ref), (init_hbm, init_ref), (two_hbm, two_ref), (three_hbm, three_ref)]
    small_loads = [pltpu.make_async_copy(source, target, load_sem.at[local_two + k]) for k, (source, target) in enumerate(small)]
    small_loads[0].start()
    small_loads[1].start()
    for load in slab_loads:
        load.start()
    small_loads[2].start()
    small_loads[3].start()

    pairs = cols // 2
    turns = sorted(range(pairs), key=lambda z: (z == 0, -abs(2 * z - pairs)))
    away = [d for d in [(near, far, flip) for flip in (1, 0) for near in reversed(range(rows // 2)) for far in turns] if any(d)]

    def there(distance):
        near, far, flip = distance
        return lax.rem(row // 2 + near, rows // 2), lax.rem(col // 2 + far, pairs) * 2 + lax.rem(col + flip, 2)

    def at(index, count):
        return pl.ds(pl.multiple_of(index * count, count), count)

    barrier = pltpu.get_barrier_semaphore()

    def greet_at(there_row, there_col):
        pl.semaphore_signal(barrier, inc=1, device_id=(there_row, there_col), device_id_type=pl.DeviceIdType.MESH)

    for distance in away:
        there_row, there_col = there(distance)
        greet_at(there_row * 2, there_col)
        greet_at(there_row * 2 + 1, there_col)
    greet_at(partner, col)

    small_loads[0].wait()
    lane = iota((fourth_len, features), 1)
    shape = (rank_four, features)
    four = dot(four_ref[...], ones_where(iota(shape, 1) % rank_four == iota(shape, 0)), ((0,), (0,)))
    four_high = four.astype(jnp.bfloat16).astype(jnp.float32)
    four_low = four - four_high
    for b in range(local_two):
        for c in range(local_three):
            keep = lane // rank_four == c * local_two + b
            part = slice((b * local_three + c) * fourth_len, (b * local_three + c + 1) * fourth_len)
            mix_high[part, :] = jnp.where(keep, four_high, 0.0).astype(jnp.bfloat16)
            mix_low[part, :] = jnp.where(keep, four_low, 0.0).astype(jnp.bfloat16)

    small_loads[1].wait()
    init_high, init_low = split(init_ref[...])
    init_both = jnp.concatenate([init_high, init_low], axis=0)
    cuts = [0, local_two // 2, local_two]
    count = len(cuts) - 1

    def span_of(k):
        return slice(cuts[k] * width, cuts[k + 1] * width)

    def pull_group(k):
        both = narrow(init_both, high_ref[:, span_of(k)])
        return both[:rank_one] + both[rank_one:] + narrow(init_high, low_ref[:, span_of(k)])

    pulled, vectors = [], []
    for k in range(count + 2):
        if k < count:
            for b in range(cuts[k], cuts[k + 1]):
                slab_loads[b].wait()
                high, low = split(slabs[b])
                high_ref[:, b * width:(b + 1) * width] = high
                low_ref[:, b * width:(b + 1) * width] = low
        if k >= 2:
            vectors.append(left_split(pulled[k - 2], mix_high[span_of(k - 2), :], mix_low[span_of(k - 2), :]))
        if 1 <= k <= count:
            pulled.append(pull_group(k - 1))
    vectors = sum(vectors[1:], vectors[0])

    def fenced(body):
        def trip(_, carry):
            body()
            return carry

        lax.fori_loop(0, 1 + me // devices, trip, 0)

    def flat(ref):
        return ref.reshape(devices * local_three, lanes)

    def deal(vectors, put):
        for c in range(local_three):
            put[pl.ds(c, devices, stride=local_three), :] = vectors[:, c * lanes:(c + 1) * lanes]

    def send(stage, k):
        put, got = puts.at[stage, k], gots.at[stage, k]

        def one(there_row, there_col):
            copy_to(put.at[there_row * cols + there_col], got.at[me], there_row, there_col, send_sem.at[stage, k], recv_sem.at[stage, k])

        @fenced
        def _():
            for flip in (1, 0):
                for h in range(2):
                    for distance in away:
                        if distance[2] == flip:
                            there_row, there_col = there(distance)
                            one(there_row * 2 + h, there_col)
            one(partner, col)

        got[me] = put[me]

    def arrive(stage, k):
        wait_for(gots.at[stage, k, pl.ds(0, devices - 1)], recv_sem.at[stage, k])

    def contract(stage, k, matrix):
        got, put = flat(gots.at[stage, k]), flat(puts.at[stage + 1, k])
        size = cols * local_three
        top, rest = split(jnp.concatenate([got[i * size:(i + 1) * size, :] for i in range(rows)], axis=1))
        result = left_split(narrow(matrix, jnp.concatenate([top, top, rest], axis=0)), lane_high[...], lane_low[...])
        for i in range(rows):
            put[i * size:(i + 1) * size, :] = result[:, i * lanes:(i + 1) * lanes]

    def triple(matrix, axis):
        high, low = split(matrix)
        return jnp.concatenate([high, low, high], axis=axis)

    def collect(stage, k):
        got = flat(gots.at[stage, k])
        return jnp.concatenate([got[pl.ds(c, devices, stride=local_three), :] for c in range(local_three)], axis=1)

    for k in range(copies):
        deal(vectors[k * devices:(k + 1) * devices], flat(puts.at[0, k]))
    small_loads[2].wait()
    small_loads[3].wait()
    pl.semaphore_wait(barrier, devices - 1)

    def send_two(k, carry):
        copy_to(two_ref, twos.at[row], lax.rem(row + k, rows), col, factor_sem.at[0], factor_sem.at[1])
        return carry

    def send_three(k, carry):
        copy_to(three_ref, threes.at[col], row, lax.rem(col + k, cols), factor_sem.at[2], factor_sem.at[3])
        return carry

    lax.fori_loop(1, rows, send_two, 0, unroll=True)
    lax.fori_loop(1, cols, send_three, 0, unroll=True)
    for k in range(copies):
        send(0, k)
    twos[row] = two_ref[...]
    threes[col] = three_ref[...]

    def hat_piece(k, count):
        part = slice(k * first_len // count, (k + 1) * first_len // count)
        hat = narrow(high_ref[part, :], mix_high[...]) + narrow(high_ref[part, :], mix_low[...]) + narrow(low_ref[part, :], mix_high[...])
        hat_high[part, :], hat_low[part, :] = split(hat)
        turn_high[:, part], turn_low[:, part] = split(hat.T)

    hat_piece(0, 4)
    wait_for(twos.at[pl.ds(0, rows - 1)], factor_sem.at[1])
    wait_for(threes.at[pl.ds(0, cols - 1)], factor_sem.at[3])
    whole_two = jnp.concatenate([twos[k] for k in range(rows)], axis=0)
    whole_three = jnp.concatenate([threes[k] for k in range(cols)], axis=0)
    store_lanes(dot(whole_two, whole_two, ((1,), (1,))), rank_four, lane_high, lane_low)
    left = triple(dot(whole_three, whole_three, ((1,), (1,))), 1)

    for k in range(copies):
        arrive(0, k)
        contract(0, k, left)
        send(1, k)
    hat_piece(1, 4)
    hat_piece(2, 4)
    hat_piece(3, 4)

    def tiles():
        for i in range(members):
            r, w = i // spans, i % spans
            yield i, slice(r * 8, (r + 1) * 8), slice(w * LANES, (w + 1) * LANES)

    def image_part(back, which):
        span = at(which, half_len)
        return left_split(back, turn_high[:, span], turn_low[:, span])

    def image_out(k):
        back = collect(1, k)
        image = image_part(back, 1 - half)
        for i, r, w in tiles():
            parts[k, i] = image[r, w]
        fenced(lambda: copy_to(parts.at[k], paired.at[k], partner, col, share_sem.at[4, k], share_sem.at[5, k]))
        return back

    def scatter(k, image):
        wait_for(paired.at[k], share_sem.at[5, k])
        for i, r, w in tiles():
            sums[k, i] = image[r, w] + paired[k, i]

        @fenced
        def _():
            for distance in away + [(0, 0, 0)]:
                there_row, there_col = there(distance)
                copy_to(sums.at[k, there_row * cols + there_col], shares.at[k, seat], there_row * 2 + 1 - half, there_col, share_sem.at[0, k], share_sem.at[1, k])

    arrive(1, 0)
    owned = image_part(image_out(0), half)
    for k in range(copies):
        if k + 1 < copies:
            arrive(1, k + 1)
            back = image_out(k + 1)
        scatter(k, owned)
        if k + 1 < copies:
            owned = image_part(back, half)

    store_lanes(whole_two, rank_four, lane_high, lane_low)
    left = triple(whole_three.T, 1)
    for k in range(copies):
        wait_for(shares.at[k], share_sem.at[1, k])
        mine[k] = jnp.sum(shares[k], axis=0)

        @fenced
        def _():
            for distance in away + [(0, 0, 0)]:
                there_row, there_col = there(distance)
                copy_to(mine.at[k], spread.at[1 - half, k, seat], there_row * 2 + 1 - half, there_col, share_sem.at[2, k], share_sem.at[3, k])

    def image_half(which, k):
        return jnp.concatenate([
            jnp.concatenate([spread[which, k, r * spans + w] for w in range(spans)], axis=1)
            for r in range(members // spans)], axis=0)

    def pull_half(which, k):
        span = at(which, half_len)
        return left_split(image_half(which, k), hat_high[span, :], hat_low[span, :])

    def pass_on(k):
        wait_for(spread.at[half, k], share_sem.at[3, k])
        fenced(lambda: copy_to(spread.at[half, k], spread.at[half, k], partner, col, image_sem.at[0, k], image_sem.at[1, k]))

    pass_on(0)
    for k in range(copies):
        vectors = pull_half(half, k)
        if k + 1 < copies:
            pass_on(k + 1)
        wait_for(spread.at[1 - half, k], image_sem.at[1, k])
        deal(vectors + pull_half(1 - half, k), flat(puts.at[2, k]))
        send(2, k)

    image = jnp.concatenate([jnp.concatenate([image_half(0, k), image_half(1, k)], axis=1) for k in range(copies)], axis=0)
    lower = dot(image, image, ((1,), (1,)))
    shape = lower.shape
    lower, inverse = eliminate(lower, ones_where(iota(shape, 0) == iota(shape, 1)), 0, rank_one * 3 // 8)
    for k in range(copies):
        arrive(2, k)
        contract(2, k, left)
        send(3, k)
    lower, inverse = eliminate(lower, inverse, rank_one * 3 // 8, rank_one)
    basis_ref[...] = dot(inverse, image, ((1,), (0,)))
    inverse_high, inverse_low = split(inverse.T)
    core = None
    for k in range(copies):
        arrive(3, k)
        part = slice(k * devices, (k + 1) * devices)
        weights = jnp.concatenate([inverse_high[part], inverse_high[part], inverse_low[part]], axis=0)
        more = lax.dot_general(triple(collect(3, k), 0), weights, (((0,), (0,)), ((), ())), preferred_element_type=jnp.float32)
        core = more if core is None else core + more
    for c in range(local_three):
        for b in range(local_two):
            core_ref[b, c] = core[(c * local_two + b) * rank_four:(c * local_two + b + 1) * rank_four, :]

    for k in range(copies):
        for stage in range(4):
            wait_for(gots.at[stage, k, pl.ds(0, devices - 1)], send_sem.at[stage, k])
        wait_for(paired.at[k], share_sem.at[4, k])
        wait_for(shares.at[k], share_sem.at[0, k])
        wait_for(shares.at[k], share_sem.at[2, k])
        wait_for(paired.at[k], image_sem.at[0, k])
    wait_for(twos.at[pl.ds(0, rows - 1)], factor_sem.at[0])
    wait_for(threes.at[pl.ds(0, cols - 1)], factor_sem.at[2])


def write_kernel(core_ref, basis_ref, core_hbm, basis_hbm, sem):
    first = pltpu.make_async_copy(core_ref, core_hbm, sem.at[0])
    second = pltpu.make_async_copy(basis_ref, basis_hbm, sem.at[1])
    first.start()
    second.start()
    first.wait()
    second.wait()


def fits(tensor, factor_two, factor_three, factor_four, factor_init):
    rows, cols = lax.axis_size("row"), lax.axis_size("col")
    devices = rows * cols
    first_len, local_two, width = tensor.shape
    fourth_len, rank_four = factor_four.shape
    rank_one = factor_init.shape[1]
    local_three = width // fourth_len
    same = factor_two.shape[1] == local_two * rows and factor_three.shape[1] == local_three * cols
    even = rows % 2 == 0 and cols % 2 == 0 and rank_one % devices == 0
    flat = local_two * rank_four == LANES and width == LANES and (local_three == 4 or local_three % 8 == 0)
    tiles = (devices // 8) * (first_len // (2 * LANES))
    return same and even and flat and first_len % (4 * LANES) == 0 and devices % 8 == 0 and tiles == devices // 2


def fused(tensor, factor_two, factor_three, factor_four, factor_init):
    rows, cols = lax.axis_size("row"), lax.axis_size("col")
    devices = rows * cols
    members = devices // 2
    first_len, local_two, width = tensor.shape
    fourth_len, rank_four = factor_four.shape
    rank_one = factor_init.shape[1]
    local_three = width // fourth_len
    lanes = local_two * rank_four
    features = local_three * lanes
    total_width = local_two * width
    copies = rank_one // devices
    wide = rows * lanes

    def f32(*shape):
        return pltpu.VMEM(shape, jnp.float32)

    def bf16(*shape):
        return pltpu.VMEM(shape, jnp.bfloat16)

    vmem, hbm = pl.BlockSpec(memory_space=pltpu.VMEM), pl.BlockSpec(memory_space=pltpu.HBM)
    shapes = (
        jax.ShapeDtypeStruct((local_two, local_three, rank_four, rank_one), jnp.float32),
        jax.ShapeDtypeStruct((rank_one, first_len), jnp.float32),
    )
    operands = [pltpu.with_memory_space_constraint(x, pltpu.HBM) for x in (tensor, factor_two, factor_three, factor_four.T, factor_init.T)]
    core, basis = pl.pallas_call(
        hooi_kernel,
        out_shape=tuple(pltpu.VMEM(x.shape, x.dtype) for x in shapes),
        in_specs=[hbm] * 5,
        out_specs=(vmem, vmem),
        scratch_shapes=[
            f32(local_two, first_len, width), f32(*factor_two.shape), f32(*factor_three.shape), f32(rank_four, fourth_len), f32(rank_one, first_len),
            bf16(first_len, total_width), bf16(first_len, total_width), bf16(total_width, features), bf16(total_width, features),
            bf16(first_len, features), bf16(first_len, features), bf16(features, first_len), bf16(features, first_len),
            bf16(wide, wide), bf16(wide, wide), f32(rows, *factor_two.shape), f32(cols, *factor_three.shape),
            f32(4, copies, devices, local_three, lanes), f32(4, copies, devices, local_three, lanes),
            f32(copies, members, 8, LANES), f32(copies, members, 8, LANES), f32(copies, members, 8, LANES), f32(copies, members, 8, LANES),
            f32(copies, 8, LANES), f32(2, copies, members, 8, LANES),
            pltpu.SemaphoreType.DMA((local_two + 4,)),
            pltpu.SemaphoreType.DMA((4,)),
            pltpu.SemaphoreType.DMA((4, copies)),
            pltpu.SemaphoreType.DMA((4, copies)),
            pltpu.SemaphoreType.DMA((2, copies)),
            pltpu.SemaphoreType.DMA((6, copies)),
        ],
        compiler_params=pltpu.CompilerParams(collective_id=0, has_side_effects=True, vmem_limit_bytes=48 << 20),
    )(*operands)
    core, basis = pl.pallas_call(
        write_kernel,
        out_shape=shapes,
        in_specs=[vmem, vmem],
        out_specs=(hbm, hbm),
        scratch_shapes=[pltpu.SemaphoreType.DMA((2,))],
        compiler_params=pltpu.CompilerParams(vmem_limit_bytes=4 << 20),
    )(core, basis)
    return basis.T, core.transpose(3, 0, 1, 2)


def shards(tensor, factor_two, factor_three, factor_four, factor_init):
    if fits(tensor, factor_two, factor_three, factor_four, factor_init):
        return fused(tensor, factor_two, factor_three, factor_four, factor_init)
    axes = ("row", "col")
    first_len, local_two, width = tensor.shape
    fourth_len, rank_four = factor_four.shape
    local_three = width // fourth_len
    rank_one = factor_init.shape[1]
    rows, cols = lax.axis_size("row"), lax.axis_size("col")
    devices = rows * cols
    local_pairs = local_two * local_three
    features = rank_four * rank_one
    part = features // devices
    data = tensor.reshape(first_len, local_pairs, fourth_len)
    rank_two, rank_three = factor_two.shape[1], factor_three.shape[1]

    def pull(vectors):
        mixed = jnp.einsum("apd,ar->prd", data, vectors, precision=lax.Precision.HIGH)
        return jnp.einsum("prd,de->per", mixed, factor_four, precision=HIGHEST).reshape(local_pairs, features)

    def share(values, ident):
        length = values.shape[1]
        padded = -(-length // LANES) * LANES
        values = jnp.pad(values, ((0, 0), (0, padded - length))).reshape(devices, padded // LANES, LANES)
        return swap(values, ident).reshape(devices, padded)[:, :length]

    def spread(block, ident, extra=None):
        put = block.reshape(local_pairs, devices, part).transpose(1, 0, 2).reshape(devices, local_pairs * part)
        if extra is not None:
            put = jnp.concatenate([put, jnp.broadcast_to(extra[None], (devices, extra.shape[0]))], axis=1)
        got = share(put, ident)
        rest = got[:, local_pairs * part:]
        got = got[:, :local_pairs * part]
        got = got.reshape(rows, cols, local_two, local_three, part)
        return got.transpose(0, 2, 1, 3, 4).reshape(rows * local_two, cols * local_three, part), rest

    def gather(block, ident):
        two, three, _ = block.shape
        put = block.reshape(rows, two // rows, cols, three // cols, part).transpose(0, 2, 1, 3, 4)
        got = share(put.reshape(devices, -1), ident).reshape(devices, (two // rows) * (three // cols), part)
        return got.transpose(1, 0, 2).reshape(got.shape[1], features)

    extra = jnp.concatenate([factor_two.reshape(-1), factor_three.reshape(-1)])
    block, rest = spread(pull(factor_init), 1, extra)
    rest = rest.reshape(rows, cols, -1)
    whole_two = rest[:, 0, :factor_two.size].reshape(-1, rank_two)
    whole_three = rest[0, :, factor_two.size:].reshape(-1, rank_three)
    block = jnp.einsum("bcq,bg->gcq", block, whole_two, precision=HIGHEST)
    block = jnp.einsum("gcq,cf->gfq", block, whole_three, precision=HIGHEST)
    block = jnp.einsum("gfq,cf->gcq", block, whole_three, precision=HIGHEST)
    block = jnp.einsum("gcq,bg->bcq", block, whole_two, precision=HIGHEST)
    block = gather(block, 2).reshape(local_pairs, rank_four, rank_one)
    block = jnp.einsum("per,de->pdr", block, factor_four, precision=HIGHEST)
    image = jnp.dot(tensor.reshape(first_len, -1), block.reshape(-1, rank_one), precision=lax.Precision.HIGH)
    half = first_len // 2
    image = jnp.concatenate([image[:half], image[half:]], axis=1).reshape(devices, half // devices, 2 * rank_one)
    image = total(image, 0).reshape(half, 2 * rank_one)
    image = jnp.concatenate([image[:, :rank_one], image[:, rank_one:]], axis=0)
    basis, inverse = finish(image)
    block, _ = spread(pull(image), 3)
    block = jnp.einsum("bcq,bg->gcq", block, whole_two, precision=HIGHEST)
    block = jnp.einsum("gcq,cf->gfq", block, whole_three, precision=HIGHEST)
    block = gather(block, 4).reshape(-1, rank_four, rank_one)
    core = jnp.einsum("per,sr->spe", block, inverse, precision=HIGHEST)
    return (basis, core.reshape(rank_one, rank_two // rows, rank_three // cols, rank_four))


def solution(mesh):
    in_specs = (P(None, "row", "col"), P("row", None), P("col", None), P(), P())
    out_specs = (P(), P(None, "row", "col", None))
    return jax.shard_map(shards, mesh=mesh, in_specs=in_specs, out_specs=out_specs, check_vma=False)
```
